32 devices in a mesh: expert: 8 (over z, core), row: 4 (over y, x).
Axes of the slice: x: 2, y: 2, z: 4, core: 2. Of those that a mesh axis runs over, the one named last changes fastest.
Arguments:
- grads: bfloat16 [8, 7168, 2048], P('expert', 'row')
- basis: bfloat16 [8, 7168, 256], P('expert', 'row'), may hold values from -0.0625 to 0.0625
- loads: int32 [8], P('expert'), may hold values from 1 to 1, as said below
- flags: int32 [8], P('expert'), may hold values 0 or 1
Outputs:
- new_basis: float32 [8, 7168, 256], P('expert', 'row')
- rotated: float32 [8, 256, 2048], P('expert', None, 'row')
The draws below stay inside these ranges and needn't reach their ends.
Inputs may be any that keep to these rules, and one draw needn't show every extreme that they name: Slots 0 to loads[d] - 1 of expert-axis index d are live and hold experts; the others are empty. Some index has all 1 slots live.
All inputs are finite; a program needn't handle non-finite values. No bound on the sum of `flags` on one device may be relied on, other than what follows from the above.
Results may differ from the reference program's by a relative error of at most 0.006.
Values sent between devices are 32-bit elements; how exact they have to be, the bound alone decides.
A program may use at most 64 MiB of HBM per device.

```python
import math
import jax
import jax.numpy as jnp
from jax import lax

D = 7168
S = 2048
K = 256
SLOTS = 1
EXPERTS = 8


def draw_grads(key, part):
    first_key, second_key = jax.random.split(jax.random.fold_in(key, 7))
    entries = jax.random.normal(first_key, (EXPERTS, D, S), jnp.float32)
    row_scale = jnp.exp(jax.random.uniform(second_key, (EXPERTS, D, 1), jnp.float32, math.log(0.5), math.log(5.0)))
    expert_ramp = 1.0 + 2.0 * jnp.arange(EXPERTS, dtype=jnp.float32) / max(EXPERTS - 1, 1)
    row_ramp = 1.0 + 2.0 * jnp.arange(D, dtype=jnp.float32) / (D - 1)
    factor = jnp.sqrt(expert_ramp)[:, None, None] * jnp.sqrt(row_ramp)[None, :, None]
    return (entries * row_scale * factor).astype(jnp.bfloat16)


def draw_loads(key, part):
    device_count = EXPERTS // SLOTS
    first_key, second_key = jax.random.split(jax.random.fold_in(key, 3))
    counts = jax.random.randint(first_key, (device_count,), 1, SLOTS + 1)
    chosen = jax.random.randint(second_key, (), 0, device_count)
    return jnp.where(jnp.arange(device_count) == chosen, SLOTS, counts).astype(jnp.int32)


def touch_ends(values, stream_key, smallest, high):
    extent = values.shape
    place = [jax.random.randint(jax.random.fold_in(stream_key, axis), (), 0, extent[axis]) for axis in range(len(extent))]
    values = values.at[tuple(place)].set(smallest)
    longest = extent.index(max(extent))
    place[longest] = (place[longest] + 1) % extent[longest]
    return values.at[tuple(place)].set(high)


def level_of(key, shape, cuts, smallest, top_value):
    factor_of, own = 1.0, jax.random.fold_in(key, 6)
    for axis_at, blocks in cuts:
        steps = jnp.exp(jax.random.uniform(jax.random.fold_in(own, axis_at), (blocks,), jnp.float32, smallest / len(cuts), top_value / len(cuts)))
        factor_of = factor_of * jnp.repeat(steps, shape[axis_at] // blocks).reshape([-1 if axis == axis_at else 1 for axis in range(len(shape))])
    return factor_of


def scatter_about(rng, shape, width, reach, cuts=(), kind=jnp.bfloat16):
    result = width * jax.random.normal(rng, shape, jnp.float32)
    if cuts:
        result = result * level_of(rng, shape, cuts, -0.22, 0.18)
    return jnp.clip(result, -reach, reach).astype(kind)


def setup_inputs(seed: int = 0) -> dict:
    streams_of = jax.random.split(jax.random.key(seed), 5)
    return {
        "grads": draw_grads(jax.random.fold_in(streams_of[4], 71), 0),
        "basis": scatter_about(streams_of[1], (EXPERTS, D, K), D ** -0.5, 0.0625, ((0, 8), (1, 4))),
        "loads": draw_loads(jax.random.fold_in(streams_of[4], 71), 0),
        "flags": touch_ends((jax.random.randint(streams_of[3], (EXPERTS,), 0, 2) < 1).astype(jnp.int32), jax.random.fold_in(streams_of[3], 1), 0, 1),
    }


def reference(grads, basis, loads, flags):
    expert_total = grads.shape[0]
    slot_count = expert_total // loads.shape[0]
    expert_ids = jnp.arange(expert_total, dtype=jnp.int32)
    live_mask = expert_ids % slot_count < loads[expert_ids // slot_count]
    refresh = jnp.logical_and(live_mask, flags == 1)

    def square_sum(expert):
        gradient = grads[expert].astype(jnp.float32)
        return jnp.sum(gradient * gradient)
    square_sums = lax.map(square_sum, expert_ids)
    total_sq = jnp.sum(jnp.where(live_mask, square_sums, 0.0))
    live_count = jnp.sum(live_mask.astype(jnp.float32))
    norm_scale = lax.rsqrt(total_sq / (live_count * D * S) + 1e-06)

    def refresh_one(expert):
        gradient = grads[expert]
        old_basis = basis[expert]
        inner_sum = jnp.dot(gradient.T.astype(jnp.float32), old_basis.astype(jnp.float32), preferred_element_type=jnp.float32).astype(jnp.bfloat16)
        power_rows = jnp.dot(gradient.astype(jnp.float32), inner_sum.astype(jnp.float32), preferred_element_type=jnp.float32).astype(jnp.bfloat16)
        ortho, upper = jnp.linalg.qr(power_rows.astype(jnp.float32))
        signs = jnp.where(jnp.diagonal(upper) < 0, -1.0, 1.0).astype(ortho.dtype)
        ortho = ortho * signs[None, :]
        fresh_rot = jnp.dot(ortho.T, gradient.astype(jnp.float32), precision=lax.Precision.HIGHEST)
        stale_rot = jnp.dot(old_basis.T.astype(jnp.float32), gradient.astype(jnp.float32), preferred_element_type=jnp.float32)
        basis_out = jnp.where(refresh[expert], ortho, jnp.where(live_mask[expert], old_basis.astype(jnp.float32), 0.0))
        rotated_out = jnp.where(refresh[expert], fresh_rot, jnp.where(live_mask[expert], stale_rot, 0.0)) * norm_scale
        return (basis_out, rotated_out)
    new_basis, rotated = lax.map(refresh_one, expert_ids)
    return (new_basis, rotated)
```

```python
import functools

import jax
import jax.numpy as jnp
from jax import lax
from jax.experimental import pallas as pl
from jax.experimental.pallas import tpu as pltpu
from jax.sharding import PartitionSpec as P

PANEL = 16
HIGHEST = lax.Precision.HIGHEST
F32 = jnp.float32
BF16 = jnp.bfloat16


def dot(a, b, precision=None):
    return lax.dot_general(a, b, (((1,), (0,)), ((), ())), precision=precision, preferred_element_type=F32)


def dot_t(a, b, precision=None):
    return lax.dot_general(a, b, (((1,), (1,)), ((), ())), precision=precision, preferred_element_type=F32)


def pieces_of(x, count):
    pieces = []
    for _ in range(count):
        pieces.append(x.astype(BF16))
        x = x - pieces[-1].astype(F32)
    return pieces


def first_bit(mask, order):
    for phase, bit in enumerate(order):
        if mask >> bit & 1:
            return phase
    return len(order)


def panel_step(work, step):
    size = work.shape[0]
    panel = work[0:PANEL, :]
    rows = lax.broadcasted_iota(jnp.int32, (PANEL, 128), 0)
    lanes = lax.broadcasted_iota(jnp.int32, (PANEL, 128), 1)
    columns = [jnp.broadcast_to(panel[:, j : j + 1], (PANEL, 128)) for j in range(PANEL)]
    pieces = [panel[:, at : at + 128] for at in range(0, size, 128)]
    unit = (rows == lanes).astype(F32)
    root = jnp.zeros((PANEL, 128), F32)
    for j in range(PANEL):
        inverse_root = lax.rsqrt(columns[j][j : j + 1, :])
        root = jnp.where(rows == j, inverse_root, root)
        factor = jnp.where(rows > j, columns[j] * (inverse_root * inverse_root), 0.0)
        for k in range(j + 1, PANEL):
            columns[k] = columns[k] - factor * columns[k][j : j + 1, :]
        pieces = [piece - factor * piece[j : j + 1, :] for piece in pieces]
        unit = unit - factor * unit[j : j + 1, :]
    scaled = [root * piece for piece in pieces]
    full = jnp.concatenate([jnp.where(lanes < PANEL, root * unit, scaled[0])] + scaled[1:], axis=1)
    where = lax.broadcasted_iota(jnp.int32, (PANEL, size), 1)
    open_columns = jnp.logical_and(where >= PANEL, where < size - PANEL * step)
    left = jnp.where(open_columns, jnp.concatenate(scaled, axis=1), 0.0)
    update = dot(left.T, full, HIGHEST)
    body = work[PANEL:, :]
    ahead = lax.broadcasted_iota(jnp.int32, body.shape, 1) < PANEL
    rest = jnp.where(ahead, 0.0, body) - update[PANEL:, :]
    work[0 : size - PANEL, :] = pltpu.roll(rest, size - PANEL, 1)
    work[size - PANEL :, :] = pltpu.roll(full, size - PANEL, 1)


def panel_steps(work, begin, end):
    def body(step, carry):
        panel_step(work, step)
        return carry

    lax.fori_loop(begin, end, body, 0)


def lower_of(work):
    shape = work.shape
    below = lax.broadcasted_iota(jnp.int32, shape, 1) <= lax.broadcasted_iota(jnp.int32, shape, 0)
    return jnp.where(below, work[...], 0.0)


def kernel(
    n, experts, entries, g_hbm, b_ref, live_ref, refresh_ref, fresh_ref, rot_ref,
    g_ref, g_sem, bt, part, land, part2, land2, full, inner, power_t, rough, power, work,
    gram, gram_land, total, total_land,
    s_rs, r_rs, s_ag, r_ag, s_rs2, r_rs2, s_gr, r_gr, s_tot, r_tot,
):
    depth, wide = g_ref.shape
    bits = n.bit_length() - 1
    expert_bits = experts.bit_length() - 1
    size = b_ref.shape[1]
    half = size // 2
    block = wide // n
    me = lax.axis_index("row")
    my_expert = lax.axis_index("expert")
    orders = [tuple(range(bits)), tuple(reversed(range(bits)))]

    def other(index, mask):
        at = index
        for bit in range(max(bits, expert_bits)):
            if mask >> bit & 1:
                at = at + (1 - 2 * (lax.rem(index // (1 << bit), 2))) * (1 << bit)
        return at

    def partner(bit):
        return {"row": other(me, 1 << bit), "expert": my_expert}

    def expert_partner(bit):
        return {"row": me, "expert": other(my_expert, 1 << bit)}

    everyone = [partner(b) for b in range(bits)] + [expert_partner(b) for b in range(expert_bits)]
    barrier = pltpu.get_barrier_semaphore()
    for peer in everyone:
        pl.semaphore_signal(barrier, inc=1, device_id=peer, device_id_type=pl.DeviceIdType.MESH)

    def columns(mask):
        return pl.ds(pl.multiple_of(other(me, mask) * block, block), block)

    def load(mask):
        return pltpu.make_async_copy(g_hbm.at[:, columns(mask)], g_ref.at[:, columns(mask)], g_sem.at[mask])

    def copy(src, dst, send, recv, to):
        return pltpu.make_async_remote_copy(
            src_ref=src, dst_ref=dst, send_sem=send, recv_sem=recv,
            device_id=to, device_id_type=pl.DeviceIdType.MESH,
        )

    moves = []
    for phase in range(bits):
        for h in range(2):
            order = orders[h]
            masks = [m for m in range(n) if first_bit(m, order) == phase]
            masks.sort(key=lambda m: first_bit(m & ~(1 << order[phase]), order))
            moves.append([(h, phase, m, m & ~(1 << order[phase])) for m in masks])
    schedule = []
    for phase in range(bits):
        a, b = moves[2 * phase], moves[2 * phase + 1]
        schedule.append([move for pair in zip(a, b) for move in pair])
    slot = {}
    for phase_moves in schedule:
        for h, phase, m, there in phase_moves:
            slot[h, phase, there] = len(slot)

    def halving(part_ref, land_ref, sends, recvs):
        def make(h, phase, m, there):
            at = slot[h, phase, there]
            return copy(part_ref.at[h, m], land_ref.at[at], sends.at[at], recvs.at[at], partner(orders[h][phase]))

        def absorb(h, phase, m):
            at = slot[h, phase, m]
            back = m | 1 << orders[h][phase]
            make(h, phase, back, m).wait_recv()
            part_ref[h, m] = part_ref[h, m] + land_ref[at]

        return make, absorb

    def begin(left_ref, part_ref, make, ensure=lambda m: None):
        started = set()
        for move in schedule[0]:
            h, _, m, _ = move
            ensure(m)
            part_ref[h, m] = dot(left_ref[h * half : (h + 1) * half, :], g_ref[:, columns(m)])
            make(*move).start()
            started.add((h, m))
        for m in range(n):
            ensure(m)
            for h in range(2):
                if (h, m) not in started:
                    part_ref[h, m] = dot(left_ref[h * half : (h + 1) * half, :], g_ref[:, columns(m)])

    def forward(make, absorb):
        for phase in range(1, bits):
            for move in schedule[phase]:
                h, _, m, _ = move
                for earlier in range(phase):
                    absorb(h, earlier, m)
                make(*move).start()

    def finish(make, absorb):
        for phase in range(bits):
            for h in range(2):
                absorb(h, phase, 0)
        for phase_moves in schedule:
            for move in phase_moves:
                make(*move).wait_send()

    def gram_exchange(between):
        for phase in range(bits):
            made = []
            for h in range(2):
                rows = slice(h * half, (h + 1) * half)
                made.append(copy(
                    gram.at[phase, rows], gram_land.at[phase, rows],
                    s_gr.at[phase, h], r_gr.at[phase, h], partner(orders[h][phase]),
                ))
            for item in made:
                item.start()
            between(phase)
            for h, item in enumerate(made):
                rows = slice(h * half, (h + 1) * half)
                item.wait_recv()
                gram[phase + 1, rows] = gram[phase, rows] + gram_land[phase, rows]
            for item in made:
                item.wait_send()

    peers = everyone

    def total_copy(at):
        return copy(total.at[at], total_land.at[at], s_tot.at[at], r_tot.at[at], peers[at])

    def total_next(at):
        total_copy(at).wait()
        total[at + 1] = total[at] + total_land[at]
        if at + 1 < len(peers):
            total_copy(at + 1).start()

    make, absorb = halving(part, land, s_rs, r_rs)
    wanted = [move[2] for move in schedule[0]] + list(range(n))
    wanted = sorted(range(n), key=wanted.index)
    for m in wanted:
        load(m).start()

    live = live_ref[0] >= 1
    refresh = refresh_ref[0] == 1

    strip = 128 if depth % 128 == 0 else depth
    for at in range(0, depth, strip):
        bt[:, at : at + strip] = b_ref[at : at + strip, :].T

    pl.semaphore_wait(barrier, len(everyone))

    loaded = []

    def ensure(m):
        if m not in loaded:
            load(m).wait()
            loaded.append(m)

    begin(bt, part, make, ensure)

    def squares_of(step, sums):
        rows = g_ref[pl.ds(pl.multiple_of(step * 16, 16), 16), :].astype(F32)
        square = rows * rows
        for at in range(0, wide, 128):
            sums = sums + square[0:8, at : at + 128] + square[8:16, at : at + 128]
        return sums

    sums = lax.fori_loop(0, depth // 16, squares_of, jnp.zeros((8, 128), F32))
    total_sq = jnp.where(live, jnp.sum(sums), 0.0)
    count = jnp.where(jnp.logical_and(live, me == 0), 1.0, 0.0)
    tile_row = lax.broadcasted_iota(jnp.int32, (8, 128), 0)
    total[0] = jnp.where(tile_row == 0, total_sq, jnp.where(tile_row == 1, count, 0.0))
    total_copy(0).start()

    forward(make, absorb)
    finish(make, absorb)

    spread = []
    for h in range(2):
        order = tuple(reversed(orders[h]))
        held = [0]
        for bit in order:
            for m in list(held):
                spread.append((h, bit, m))
                held.append(m | 1 << bit)
    number = {(h, m | 1 << bit): at for at, (h, bit, m) in enumerate(spread)}

    def spread_copy(h, bit, m):
        at = number[h, m | 1 << bit]
        src = part.at[h, 0] if m == 0 else full.at[h, m]
        return copy(src, full.at[h, m | 1 << bit], s_ag.at[at], r_ag.at[at], partner(bit))

    arrived = set()

    def take(h, m):
        if m == 0 or (h, m) in arrived:
            return
        arrived.add((h, m))
        bit = next(b for (hh, b, mm) in spread if hh == h and mm | 1 << b == m)
        spread_copy(h, bit, m & ~(1 << bit)).wait_recv()

    def keep(h, m):
        source = part[h, 0] if m == 0 else full[h, m]
        inner[columns(m), h * half : (h + 1) * half] = source.T.astype(BF16)

    rank = {0: [], 1: []}
    for h, bit, m in spread:
        if m == 0:
            rank[h].append((h, bit, m))
    for pair in zip(rank[0], rank[1]):
        for item in pair:
            spread_copy(*item).start()
    panels = size // PANEL
    total_next(0)
    for h, bit, m in sorted((s for s in spread if s[2]), key=lambda s: bin(s[2]).count("1")):
        take(h, m)
        spread_copy(h, bit, m).start()
    tile = 256 if depth % 256 == 0 else 64
    masks = sorted(range(n), key=lambda v: bin(v).count("1"))
    for m in masks:
        for h in range(2):
            take(h, m)
            keep(h, m)
        if m == masks[-1]:
            break
        for at in range(0, depth, tile):
            rows = slice(at, at + tile)
            term = dot(g_ref[rows, columns(m)], inner[columns(m), :])
            rough[rows, :] = term if m == 0 else rough[rows, :] + term
    for at in range(0, depth, tile):
        rows = slice(at, at + tile)
        last = dot(g_ref[rows, columns(masks[-1])], inner[columns(masks[-1]), :])
        power[rows, :] = (rough[rows, :] + last).astype(BF16)
        power_t[:, rows] = power[rows, :].T
    gram[0] = dot_t(power_t[...], power_t[...])
    for item in spread:
        spread_copy(*item).wait_send()
    if len(peers) > 1:
        total_next(1)

    make2, absorb2 = halving(part2, land2, s_rs2, r_rs2)

    def cross_part(h, m):
        part2[h, m] = dot(power_t[h * half : (h + 1) * half, :], g_ref[:, columns(m)])

    def beside(phase):
        if phase == 0:
            for h, _, m, _ in schedule[0]:
                cross_part(h, m)
        if phase == bits - 1:
            for move in schedule[0]:
                make2(*move).start()
            started = [(move[0], move[2]) for move in schedule[0]]
            for h, m in [(h, m) for m in range(n) for h in range(2)]:
                if (h, m) not in started:
                    cross_part(h, m)

    gram_exchange(beside)
    for at in range(2, len(peers) - 1):
        total_next(at)
    work[...] = gram[bits]
    panel_steps(work, 0, panels // 2)
    forward(make2, absorb2)
    panel_steps(work, panels // 2, panels)
    inverse = lower_of(work)
    turn = pieces_of(inverse.T, 3)
    for at in range(0, depth, tile):
        rows = slice(at, at + tile)
        fresh = dot(power[rows, :], turn[2]) + dot(power[rows, :], turn[1]) + dot(power[rows, :], turn[0])
        fresh_ref[rows, :] = jnp.where(refresh, fresh, jnp.where(live, b_ref[rows, :].astype(F32), 0.0))
    if len(peers) > 2:
        total_next(len(peers) - 1)
    final = total[len(peers)]
    norm = lax.rsqrt(final[0:1, 0:1] / (final[1:2, 0:1] * entries) + 1e-6)
    finish(make2, absorb2)
    cross = jnp.concatenate([part2[0, 0], part2[1, 0]], axis=0)
    stale = jnp.concatenate([part[0, 0], part[1, 0]], axis=0)
    turned = dot(inverse, cross, HIGHEST)
    rot_ref[...] = jnp.where(refresh, turned, jnp.where(live, stale, 0.0)) * norm


def on_device(n, experts, grads, basis, loads, flags):
    _, depth, wide = grads.shape
    size = basis.shape[2]
    block = wide // n
    bits = n.bit_length() - 1
    peers = bits + experts.bit_length() - 1
    moves = 2 * (n - 1)
    live = loads
    refresh = jnp.where(loads >= 1, flags, 0)
    vmem = pl.BlockSpec(memory_space=pltpu.VMEM)
    smem = pl.BlockSpec(memory_space=pltpu.SMEM)
    chunk = (size // 2, block)
    dma = pltpu.SemaphoreType.DMA
    new_basis, rotated = pl.pallas_call(
        functools.partial(kernel, n, experts, float(depth * n * wide)),
        out_shape=(
            jax.ShapeDtypeStruct((depth, size), F32),
            jax.ShapeDtypeStruct((size, block), F32),
        ),
        in_specs=[pl.BlockSpec(memory_space=pl.ANY), vmem, smem, smem],
        out_specs=(vmem, vmem),
        scratch_shapes=[
            pltpu.VMEM((depth, wide), BF16),
            pltpu.SemaphoreType.DMA((n,)),
            pltpu.VMEM((size, depth), BF16),
            pltpu.VMEM((2, n, *chunk), F32),
            pltpu.VMEM((moves, *chunk), F32),
            pltpu.VMEM((2, n, *chunk), F32),
            pltpu.VMEM((moves, *chunk), F32),
            pltpu.VMEM((2, n, *chunk), F32),
            pltpu.VMEM((wide, size), BF16),
            pltpu.VMEM((size, depth), BF16),
            pltpu.VMEM((depth, size), F32),
            pltpu.VMEM((depth, size), BF16),
            pltpu.VMEM((size, size), F32),
            pltpu.VMEM((bits + 1, size, size), F32),
            pltpu.VMEM((bits, size, size), F32),
            pltpu.VMEM((peers + 1, 8, 128), F32),
            pltpu.VMEM((peers, 8, 128), F32),
            dma((moves,)), dma((moves,)), dma((moves,)), dma((moves,)), dma((moves,)), dma((moves,)),
            dma((bits, 2)), dma((bits, 2)), dma((peers,)), dma((peers,)),
        ],
        compiler_params=pltpu.CompilerParams(
            collective_id=0, has_side_effects=True, vmem_limit_bytes=58 * 1024 * 1024
        ),
    )(grads[0], basis[0], live, refresh)
    return new_basis[None], rotated[None]


def solution(mesh):
    placed = (P("expert", "row", None), P("expert", "row", None), P("expert"), P("expert"))
    return jax.shard_map(
        functools.partial(on_device, mesh.shape["row"], mesh.shape["expert"]),
        mesh=mesh,
        in_specs=placed,
        out_specs=(P("expert", "row", None), P("expert", None, "row")),
        check_vma=False,
    )
```

```python
import functools

import jax
import jax.numpy as jnp
from jax import lax
from jax.experimental import pallas as pl
from jax.experimental.pallas import tpu as pltpu
from jax.sharding import PartitionSpec as P

PANEL = 16
HIGHEST = lax.Precision.HIGHEST
F32 = jnp.float32
BF16 = jnp.bfloat16


def dot(a, b, precision=None):
    return lax.dot_general(a, b, (((1,), (0,)), ((), ())), precision=precision, preferred_element_type=F32)


def dot_t(a, b, precision=None):
    return lax.dot_general(a, b, (((1,), (1,)), ((), ())), precision=precision, preferred_element_type=F32)


def pieces_of(x, count):
    pieces = []
    for _ in range(count):
        pieces.append(x.astype(BF16))
        x = x - pieces[-1].astype(F32)
    return pieces


def first_bit(mask, order):
    for phase, bit in enumerate(order):
        if mask >> bit & 1:
            return phase
    return len(order)


def panel_step(work, step):
    size = work.shape[0]
    panel = work[0:PANEL, :]
    rows = lax.broadcasted_iota(jnp.int32, (PANEL, 128), 0)
    lanes = lax.broadcasted_iota(jnp.int32, (PANEL, 128), 1)
    columns = [jnp.broadcast_to(panel[:, j : j + 1], (PANEL, 128)) for j in range(PANEL)]
    pieces = [panel[:, at : at + 128] for at in range(0, size, 128)]
    unit = (rows == lanes).astype(F32)
    root = jnp.zeros((PANEL, 128), F32)
    for j in range(PANEL):
        inverse_root = lax.rsqrt(columns[j][j : j + 1, :])
        root = jnp.where(rows == j, inverse_root, root)
        factor = jnp.where(rows > j, columns[j] * (inverse_root * inverse_root), 0.0)
        for k in range(j + 1, PANEL):
            columns[k] = columns[k] - factor * columns[k][j : j + 1, :]
        pieces = [piece - factor * piece[j : j + 1, :] for piece in pieces]
        unit = unit - factor * unit[j : j + 1, :]
    scaled = [root * piece for piece in pieces]
    full = jnp.concatenate([jnp.where(lanes < PANEL, root * unit, scaled[0])] + scaled[1:], axis=1)
    where = lax.broadcasted_iota(jnp.int32, (PANEL, size), 1)
    open_columns = jnp.logical_and(where >= PANEL, where < size - PANEL * step)
    left = jnp.where(open_columns, jnp.concatenate(scaled, axis=1), 0.0)
    update = dot(left.T, full, HIGHEST)
    body = work[PANEL:, :]
    ahead = lax.broadcasted_iota(jnp.int32, body.shape, 1) < PANEL
    rest = jnp.where(ahead, 0.0, body) - update[PANEL:, :]
    work[0 : size - PANEL, :] = pltpu.roll(rest, size - PANEL, 1)
    work[size - PANEL :, :] = pltpu.roll(full, size - PANEL, 1)


def panel_steps(work, begin, end):
    def body(step, carry):
        panel_step(work, step)
        return carry

    lax.fori_loop(begin, end, body, 0)


def lower_of(work):
    shape = work.shape
    below = lax.broadcasted_iota(jnp.int32, shape, 1) <= lax.broadcasted_iota(jnp.int32, shape, 0)
    return jnp.where(below, work[...], 0.0)


def kernel(
    n, experts, entries, g_hbm, b_hbm, loads_hbm, flags_hbm, fresh_hbm, rot_hbm,
    g_ref, b_ref, bt, part, land, full, inner, rough, power, part2, land2,
    gram_a, gram_a_land, gram_b, gram_b_land, work, fresh, rot, total, total_land, loads, flags,
    g_sem, b_sem, in_sem, out_sem,
    s_rs, r_rs, s_ag, r_ag, s_rs2, r_rs2, s_gr, r_gr, s_tot, r_tot,
):
    _, depth, block = g_ref.shape
    bits = n.bit_length() - 1
    expert_bits = experts.bit_length() - 1
    size = b_ref.shape[1]
    half = size // 2
    sub = half // 2
    me = lax.axis_index("row")
    my_expert = lax.axis_index("expert")
    orders = [tuple(range(bits)), tuple(reversed(range(bits)))]

    def other(index, mask):
        at = index
        for bit in range(max(bits, expert_bits)):
            if mask >> bit & 1:
                at = at + (1 - 2 * (lax.rem(index // (1 << bit), 2))) * (1 << bit)
        return at

    def partner(bit):
        return {"row": other(me, 1 << bit), "expert": my_expert}

    def expert_partner(bit):
        return {"row": me, "expert": other(my_expert, 1 << bit)}

    peers = [partner(b) for b in range(bits)] + [expert_partner(b) for b in range(expert_bits)]
    barrier = pltpu.get_barrier_semaphore()
    for peer in peers:
        pl.semaphore_signal(barrier, inc=1, device_id=peer, device_id_type=pl.DeviceIdType.MESH)

    def load(m):
        columns = pl.ds(pl.multiple_of(other(me, m) * block, block), block)
        return pltpu.make_async_copy(g_hbm.at[:, columns], g_ref.at[m], g_sem.at[m])

    def load_basis(a):
        columns = pl.ds(a * half, half)
        return pltpu.make_async_copy(b_hbm.at[:, columns], b_ref.at[:, columns], b_sem.at[a])

    def copy(src, dst, send, recv, to):
        return pltpu.make_async_remote_copy(
            src_ref=src, dst_ref=dst, send_sem=send, recv_sem=recv,
            device_id=to, device_id_type=pl.DeviceIdType.MESH,
        )

    def strip(h):
        return pl.ds(h * sub, sub)

    schedule = []
    for phase in range(bits):
        lanes = []
        for h in range(2):
            order = orders[h]
            masks = [m for m in range(n) if first_bit(m, order) == phase]
            masks.sort(key=lambda m: first_bit(m & ~(1 << order[phase]), order))
            lanes.append([(h, phase, m, m & ~(1 << order[phase])) for m in masks])
        schedule.append([move for pair in zip(*lanes) for move in pair])
    slot = {}
    for phase_moves in schedule:
        for h, phase, m, there in phase_moves:
            slot[h, phase, there] = len(slot)

    class Halving:
        def __init__(self, a, parts, lands, sends, recvs):
            self.a, self.parts, self.lands, self.sends, self.recvs = a, parts, lands, sends, recvs

        def make(self, h, phase, m, there):
            at = slot[h, phase, there]
            return copy(
                self.parts.at[self.a, m, strip(h)], self.lands.at[self.a, at],
                self.sends.at[self.a, at], self.recvs.at[self.a, at], partner(orders[h][phase]),
            )

        def absorb(self, h, phase, m):
            self.make(h, phase, m | 1 << orders[h][phase], m).wait_recv()
            rows = slice(h * sub, (h + 1) * sub)
            self.parts[self.a, m, rows] = self.parts[self.a, m, rows] + self.lands[self.a, slot[h, phase, m]]

        def send(self, moves):
            for move in moves:
                self.make(*move).start()

        def forward(self):
            for phase in range(1, bits):
                for move in schedule[phase]:
                    for earlier in range(phase):
                        self.absorb(move[0], earlier, move[2])
                    self.make(*move).start()

        def finish(self):
            for phase in range(bits):
                for h in range(2):
                    self.absorb(h, phase, 0)

        def drain(self):
            for phase_moves in schedule:
                for move in phase_moves:
                    self.make(*move).wait_send()

    first = [Halving(a, part, land, s_rs, r_rs) for a in range(2)]
    second = [Halving(a, part2, land2, s_rs2, r_rs2) for a in range(2)]

    spread = []
    for h in range(2):
        held = [0]
        for bit in reversed(orders[h]):
            for m in list(held):
                spread.append((h, bit, m))
                held.append(m | 1 << bit)
    number = {(h, m | 1 << bit): at for at, (h, bit, m) in enumerate(spread)}
    source = {(h, m | 1 << bit): (h, bit, m) for h, bit, m in spread}
    own = [item for pair in zip(*[[s for s in spread if s[0] == h and s[2] == 0] for h in range(2)]) for item in pair]
    relayed = sorted((s for s in spread if s[2]), key=lambda s: bin(s[2]).count("1"))

    def spread_copy(a, h, bit, m):
        at = number[h, m | 1 << bit]
        src = part.at[a, 0, strip(h)] if m == 0 else full.at[a, m, strip(h)]
        return copy(src, full.at[a, m | 1 << bit, strip(h)], s_ag.at[a, at], r_ag.at[a, at], partner(bit))

    arrived = set()

    def take(a, h, m):
        if m and (a, h, m) not in arrived:
            arrived.add((a, h, m))
            spread_copy(a, *source[h, m]).wait_recv()

    def relay(a):
        for h, bit, m in relayed:
            take(a, h, m)
            spread_copy(a, h, bit, m).start()

    tile = 256 if depth % 256 == 0 else 64
    masks = sorted(range(n), key=lambda v: bin(v).count("1"))

    def add_power(a, m):
        for h in range(2):
            take(a, h, m)
        held = part[a, 0] if m == 0 else full[a, m]
        inner[a, m] = held.astype(BF16)
        for at in range(0, depth, tile):
            rows = slice(at, at + tile)
            term = dot_t(inner[a, m], g_ref[m, rows, :])
            if m:
                term = rough[a, :, rows] + term
            if m == masks[-1]:
                power[a * half : (a + 1) * half, rows] = term.astype(BF16)
            else:
                rough[a, :, rows] = term

    grams = [(gram_a, gram_a_land), (gram_b, gram_b_land)]

    def gram_copy(a, phase, h):
        held, landed = grams[a]
        extent = held.shape[1] // 2
        rows = pl.ds(h * extent, extent)
        return copy(
            held.at[phase, rows], landed.at[phase, rows],
            s_gr.at[a, phase, h], r_gr.at[a, phase, h], partner(orders[h][phase]),
        )

    def gram_send(a, phase):
        for h in range(2):
            gram_copy(a, phase, h).start()

    def gram_add(a, phase):
        held, landed = grams[a]
        extent = held.shape[1] // 2
        for h in range(2):
            rows = slice(h * extent, (h + 1) * extent)
            gram_copy(a, phase, h).wait_recv()
            held[phase + 1, rows] = held[phase, rows] + landed[phase, rows]

    def total_copy(at):
        return copy(total.at[at], total_land.at[at], s_tot.at[at], r_tot.at[at], peers[at])

    def total_next(at):
        if at >= len(peers):
            return
        total_copy(at).wait()
        total[at + 1] = total[at] + total_land[at]
        if at + 1 < len(peers):
            total_copy(at + 1).start()

    wanted = [move[2] for move in schedule[0]] + list(range(n))
    wanted = sorted(range(n), key=wanted.index)
    load_basis(0).start()
    load(wanted[0]).start()
    load_basis(1).start()
    for m in wanted[1:]:
        load(m).start()
    small = [
        pltpu.make_async_copy(loads_hbm, loads, in_sem.at[0]),
        pltpu.make_async_copy(flags_hbm, flags, in_sem.at[1]),
    ]
    for item in small:
        item.start()

    span = 128 if depth % 128 == 0 else depth

    def turn_basis(a):
        load_basis(a).wait()
        for at in range(0, depth, span):
            bt[a * half : (a + 1) * half, at : at + span] = b_ref[at : at + span, a * half : (a + 1) * half].T

    turn_basis(0)
    pl.semaphore_wait(barrier, len(peers))
    for m in wanted:
        load(m).wait()
        part[0, m] = dot(bt[0:half, :], g_ref[m])
        first[0].send([move for move in schedule[0] if move[2] == m])
    turn_basis(1)
    for m in wanted:
        part[1, m] = dot(bt[half:size, :], g_ref[m])
    first[0].forward()
    first[1].send(schedule[0])

    for item in small:
        item.wait()
    live = loads[0] >= 1
    refresh = jnp.logical_and(live, flags[0] == 1)

    def squares_of(step, sums):
        rows = pl.ds(pl.multiple_of(step * 16, 16), 16)
        for m in range(n):
            piece = g_ref[m, rows, :].astype(F32)
            sums = sums + piece * piece
        return sums

    sums = lax.fori_loop(0, depth // 16, squares_of, jnp.zeros((16, block), F32))
    total_sq = jnp.where(live, jnp.sum(sums), 0.0)
    count = jnp.where(jnp.logical_and(live, me == 0), 1.0, 0.0)
    tile_row = lax.broadcasted_iota(jnp.int32, (8, 128), 0)
    total[0] = jnp.where(tile_row == 0, total_sq, jnp.where(tile_row == 1, count, 0.0))
    total_copy(0).start()

    first[0].finish()
    for item in own[:2]:
        spread_copy(0, *item).start()
    first[1].forward()
    for item in own[2:]:
        spread_copy(0, *item).start()
    add_power(0, 0)
    relay(0)
    first[1].finish()
    for item in own:
        spread_copy(1, *item).start()
    total_next(0)
    add_power(1, 0)
    for m in masks[1:]:
        add_power(0, m)
    gram_a[0] = dot_t(power[0:half, :], power[0:half, :])
    gram_send(0, 0)

    def cross_part(a):
        for m in wanted:
            part2[a, m] = dot(power[a * half : (a + 1) * half, :], g_ref[m])

    cross_part(0)
    total_next(1)
    relay(1)
    second[0].send(schedule[0][:2])
    for phase in range(bits - 1):
        gram_add(0, phase)
        gram_send(0, phase + 1)
    second[0].send(schedule[0][2:])
    total_next(2)
    for m in masks[1:]:
        add_power(1, m)
    gram_b[0] = dot_t(power[...], power[half:size, :])
    gram_send(1, 0)
    gram_add(0, bits - 1)
    panels = half // PANEL
    work[...] = gram_a[bits]
    panel_steps(work, 0, panels // 2)
    second[0].forward()
    cross_part(1)
    panel_steps(work, panels // 2, panels)
    for phase in range(bits - 1):
        gram_add(1, phase)
        gram_send(1, phase + 1)
    second[1].send(schedule[0])
    total_next(3)

    def write_fresh(a, pieces):
        for at in range(0, depth, tile):
            rows = slice(at, at + tile)
            columns = slice(a * half, (a + 1) * half)
            left = power[0 : (a + 1) * half, rows].T
            value = dot(left, pieces[2]) + dot(left, pieces[1]) + dot(left, pieces[0])
            kept = jnp.where(live, b_ref[rows, columns].astype(F32), 0.0)
            fresh[a, rows, :] = jnp.where(refresh, value, kept)
        fresh_out(a).start()

    def fresh_out(a):
        return pltpu.make_async_copy(fresh.at[a], fresh_hbm.at[:, pl.ds(a * half, half)], out_sem.at[a])

    def rot_out(a):
        rows = pl.ds(a * half, half)
        return pltpu.make_async_copy(rot.at[rows], rot_hbm.at[rows], out_sem.at[2 + a])

    inverse_a = lower_of(work)
    write_fresh(0, pieces_of(inverse_a.T, 3))
    second[0].finish()
    turned_a = dot(inverse_a, part2[0, 0], HIGHEST)
    gram_add(1, bits - 1)
    upper = dot(inverse_a, gram_b[bits, 0:half], HIGHEST)
    work[...] = gram_b[bits, half:size] - dot(upper.T, upper, HIGHEST)
    panel_steps(work, 0, panels // 2)
    second[1].forward()
    panel_steps(work, panels // 2, panels)
    inverse_b = lower_of(work)
    mixed = -dot(inverse_b, dot(upper.T, inverse_a, HIGHEST), HIGHEST)
    write_fresh(1, pieces_of(jnp.concatenate([mixed, inverse_b], axis=1).T, 3))
    partly = dot(mixed, part2[0, 0], HIGHEST)
    for at in range(4, len(peers)):
        total_next(at)
    final = total[len(peers)]
    norm = lax.rsqrt(final[0:1, 0:1] / (final[1:2, 0:1] * entries) + 1e-6)

    def write_rot(a, turned):
        value = jnp.where(refresh, turned, jnp.where(live, part[a, 0], 0.0)) * norm
        rot[a * half : (a + 1) * half, :] = value
        rot_out(a).start()

    write_rot(0, turned_a)
    second[1].finish()
    write_rot(1, partly + dot(inverse_b, part2[1, 0], HIGHEST))
    for a in range(2):
        first[a].drain()
        second[a].drain()
        for item in spread:
            spread_copy(a, *item).wait_send()
        for phase in range(bits):
            for h in range(2):
                gram_copy(a, phase, h).wait_send()
        fresh_out(a).wait()
    for a in range(2):
        rot_out(a).wait()


def on_device(n, experts, grads, basis, loads, flags):
    _, depth, wide = grads.shape
    size = basis.shape[2]
    half = size // 2
    block = wide // n
    bits = n.bit_length() - 1
    peers = bits + experts.bit_length() - 1
    moves = 2 * (n - 1)
    anywhere = pl.BlockSpec(memory_space=pl.ANY)
    chunk = (half // 2, block)
    dma = pltpu.SemaphoreType.DMA
    new_basis, rotated = pl.pallas_call(
        functools.partial(kernel, n, experts, float(depth * n * wide)),
        out_shape=(
            jax.ShapeDtypeStruct((depth, size), F32),
            jax.ShapeDtypeStruct((size, block), F32),
        ),
        in_specs=[anywhere] * 4,
        out_specs=(anywhere, anywhere),
        scratch_shapes=[
            pltpu.VMEM((n, depth, block), BF16),
            pltpu.VMEM((depth, size), BF16),
            pltpu.VMEM((size, depth), BF16),
            pltpu.VMEM((2, n, half, block), F32),
            pltpu.VMEM((2, moves, *chunk), F32),
            pltpu.VMEM((2, n, half, block), F32),
            pltpu.VMEM((2, n, half, block), BF16),
            pltpu.VMEM((2, half, depth), F32),
            pltpu.VMEM((size, depth), BF16),
            pltpu.VMEM((2, n, half, block), F32),
            pltpu.VMEM((2, moves, *chunk), F32),
            pltpu.VMEM((bits + 1, half, half), F32),
            pltpu.VMEM((bits, half, half), F32),
            pltpu.VMEM((bits + 1, size, half), F32),
            pltpu.VMEM((bits, size, half), F32),
            pltpu.VMEM((half, half), F32),
            pltpu.VMEM((2, depth, half), F32),
            pltpu.VMEM((size, block), F32),
            pltpu.VMEM((peers + 1, 8, 128), F32),
            pltpu.VMEM((peers, 8, 128), F32),
            pltpu.SMEM((1,), jnp.int32),
            pltpu.SMEM((1,), jnp.int32),
            dma((n,)), dma((2,)), dma((2,)), dma((4,)),
            dma((2, moves)), dma((2, moves)), dma((2, moves)), dma((2, moves)), dma((2, moves)), dma((2, moves)),
            dma((2, bits, 2)), dma((2, bits, 2)), dma((peers,)), dma((peers,)),
        ],
        compiler_params=pltpu.CompilerParams(
            collective_id=0, has_side_effects=True, vmem_limit_bytes=58 * 1024 * 1024
        ),
    )(grads[0], basis[0], loads, flags)
    return new_basis[None], rotated[None]


def solution(mesh):
    placed = (P("expert", "row", None), P("expert", "row", None), P("expert"), P("expert"))
    return jax.shard_map(
        functools.partial(on_device, mesh.shape["row"], mesh.shape["expert"]),
        mesh=mesh,
        in_specs=placed,
        out_specs=(P("expert", "row", None), P("expert", None, "row")),
        check_vma=False,
    )
```

```python
import functools

import jax
import jax.numpy as jnp
from jax import lax
from jax.experimental import pallas as pl
from jax.experimental.pallas import tpu as pltpu
from jax.sharding import PartitionSpec as P

PANEL = 16
PARTS = 4
SWAP, ACROSS, OUTWARD = range(3)
HIGHEST = lax.Precision.HIGHEST
F32 = jnp.float32
BF16 = jnp.bfloat16


def dot(a, b, precision=None):
    return lax.dot_general(a, b, (((1,), (0,)), ((), ())), precision=precision, preferred_element_type=F32)


def dot_t(a, b, precision=None):
    return lax.dot_general(a, b, (((1,), (1,)), ((), ())), precision=precision, preferred_element_type=F32)


def pieces_of(x, count):
    pieces = []
    for _ in range(count):
        pieces.append(x.astype(BF16))
        x = x - pieces[-1].astype(F32)
    return pieces


def first_bit(mask, order):
    for phase, bit in enumerate(order):
        if mask >> bit & 1:
            return phase
    return len(order)


def panel_step(work, step):
    size = work.shape[0]
    panel = work[0:PANEL, :]
    rows = lax.broadcasted_iota(jnp.int32, (PANEL, 128), 0)
    lanes = lax.broadcasted_iota(jnp.int32, (PANEL, 128), 1)
    columns = [jnp.broadcast_to(panel[:, j : j + 1], (PANEL, 128)) for j in range(PANEL)]
    pieces = [panel[:, at : at + 128] for at in range(0, size, 128)]
    unit = (rows == lanes).astype(F32)
    root = jnp.zeros((PANEL, 128), F32)
    for j in range(PANEL):
        inverse_root = lax.rsqrt(columns[j][j : j + 1, :])
        root = jnp.where(rows == j, inverse_root, root)
        factor = jnp.where(rows > j, columns[j] * (inverse_root * inverse_root), 0.0)
        for k in range(j + 1, PANEL):
            columns[k] = columns[k] - factor * columns[k][j : j + 1, :]
        pieces = [piece - factor * piece[j : j + 1, :] for piece in pieces]
        unit = unit - factor * unit[j : j + 1, :]
    scaled = [root * piece for piece in pieces]
    full = jnp.concatenate([jnp.where(lanes < PANEL, root * unit, scaled[0])] + scaled[1:], axis=1)
    where = lax.broadcasted_iota(jnp.int32, (PANEL, size), 1)
    open_columns = jnp.logical_and(where >= PANEL, where < size - PANEL * step)
    left = jnp.where(open_columns, jnp.concatenate(scaled, axis=1), 0.0)
    update = dot(left.T, full, HIGHEST)
    body = work[PANEL:, :]
    ahead = lax.broadcasted_iota(jnp.int32, body.shape, 1) < PANEL
    rest = jnp.where(ahead, 0.0, body) - update[PANEL:, :]
    work[0 : size - PANEL, :] = pltpu.roll(rest, size - PANEL, 1)
    work[size - PANEL :, :] = pltpu.roll(full, size - PANEL, 1)


def panel_steps(work, begin, end):
    def body(step, carry):
        panel_step(work, step)
        return carry

    lax.fori_loop(begin, end, body, 0)


def lower_of(work):
    shape = work.shape
    below = lax.broadcasted_iota(jnp.int32, shape, 1) <= lax.broadcasted_iota(jnp.int32, shape, 0)
    return jnp.where(below, work[...], 0.0)


def kernel(
    n, experts, entries, g_hbm, b_hbm, loads, flags, fresh, rot,
    g_ref, b_ref, bt, part, land, full, inner, rough, power, part2, land2,
    gram_a, gram_a_land, gram_b, gram_b_land, work, total, total_land,
    g_sem, b_sem,
    s_rs, r_rs, s_ag, r_ag, s_rs2, r_rs2, s_gr, r_gr, s_tot, r_tot,
):
    _, depth, block = g_ref.shape
    bits = n.bit_length() - 1
    expert_bits = experts.bit_length() - 1
    size = b_ref.shape[1]
    half = size // 2
    sub = half // 2
    me = lax.axis_index("row")
    my_expert = lax.axis_index("expert")
    orders = [tuple(range(bits)), tuple(reversed(range(bits)))]

    def other(index, mask):
        at = index
        for bit in range(max(bits, expert_bits)):
            if mask >> bit & 1:
                at = at + (1 - 2 * (lax.rem(index // (1 << bit), 2))) * (1 << bit)
        return at

    def partner(bit):
        return {"row": other(me, 1 << bit), "expert": my_expert}

    def expert_partner(bit):
        return {"row": me, "expert": other(my_expert, 1 << bit)}

    place = my_expert // 2
    inside = jnp.logical_or(place == 1, place == 2)
    across = {"row": me, "expert": my_expert + jnp.where(place == 1, 2, -2)}
    if expert_bits == 3:
        rounds = [(SWAP, expert_partner(0)), (SWAP, expert_partner(1)), (ACROSS, across), (OUTWARD, expert_partner(1))]
    else:
        rounds = [(SWAP, expert_partner(b)) for b in range(expert_bits)]
    rounds = rounds + [(SWAP, partner(b)) for b in range(bits)]
    barrier = pltpu.get_barrier_semaphore()

    def greet(peer):
        pl.semaphore_signal(barrier, inc=1, device_id=peer, device_id_type=pl.DeviceIdType.MESH)

    greetings = 0
    for kind, peer in rounds:
        if kind == SWAP:
            greet(peer)
            greetings += 1
    if expert_bits == 3:
        pl.when(inside)(lambda: greet(across))
        greetings = greetings + inside.astype(jnp.int32)

    def load(m):
        columns = pl.ds(pl.multiple_of(other(me, m) * block, block), block)
        return pltpu.make_async_copy(g_hbm.at[:, columns], g_ref.at[m], g_sem.at[m])

    def load_basis(a):
        columns = pl.ds(a * half, half)
        return pltpu.make_async_copy(b_hbm.at[:, columns], b_ref.at[:, columns], b_sem.at[a])

    def copy(src, dst, send, recv, to):
        return pltpu.make_async_remote_copy(
            src_ref=src, dst_ref=dst, send_sem=send, recv_sem=recv,
            device_id=to, device_id_type=pl.DeviceIdType.MESH,
        )

    def strip(h):
        return pl.ds(h * sub, sub)

    schedule = []
    for phase in range(bits):
        lanes = []
        for h in range(2):
            order = orders[h]
            masks = [m for m in range(n) if first_bit(m, order) == phase]
            masks.sort(key=lambda m: first_bit(m & ~(1 << order[phase]), order))
            lanes.append([(h, phase, m, m & ~(1 << order[phase])) for m in masks])
        schedule.append([move for pair in zip(*lanes) for move in pair])
    slot = {}
    for phase_moves in schedule:
        for h, phase, m, there in phase_moves:
            slot[h, phase, there] = len(slot)

    class Halving:
        def __init__(self, a, parts, lands, sends, recvs):
            self.a, self.parts, self.lands, self.sends, self.recvs = a, parts, lands, sends, recvs

        def make(self, h, phase, m, there):
            at = slot[h, phase, there]
            return copy(
                self.parts.at[self.a, m, strip(h)], self.lands.at[self.a, at],
                self.sends.at[self.a, at], self.recvs.at[self.a, at], partner(orders[h][phase]),
            )

        def absorb(self, h, phase, m):
            self.make(h, phase, m | 1 << orders[h][phase], m).wait_recv()
            rows = slice(h * sub, (h + 1) * sub)
            self.parts[self.a, m, rows] = self.parts[self.a, m, rows] + self.lands[self.a, slot[h, phase, m]]

        def send(self, moves):
            for move in moves:
                self.make(*move).start()

        def forward(self):
            for phase in range(1, bits):
                for move in schedule[phase]:
                    for earlier in range(phase):
                        self.absorb(move[0], earlier, move[2])
                    self.make(*move).start()

        def finish(self):
            for phase in range(bits):
                for h in range(2):
                    self.absorb(h, phase, 0)

        def drain(self):
            for phase_moves in schedule:
                for move in phase_moves:
                    self.make(*move).wait_send()

    first = [Halving(a, part, land, s_rs, r_rs) for a in range(2)]
    second = [Halving(a, part2, land2, s_rs2, r_rs2) for a in range(2)]

    spread = []
    for h in range(2):
        held = [0]
        for bit in reversed(orders[h]):
            for m in list(held):
                spread.append((h, bit, m))
                held.append(m | 1 << bit)
    number = {(h, m | 1 << bit): at for at, (h, bit, m) in enumerate(spread)}
    source = {(h, m | 1 << bit): (h, bit, m) for h, bit, m in spread}
    own = [item for pair in zip(*[[s for s in spread if s[0] == h and s[2] == 0] for h in range(2)]) for item in pair]
    relayed = sorted((s for s in spread if s[2]), key=lambda s: bin(s[2]).count("1"))

    def spread_copy(a, h, bit, m):
        at = number[h, m | 1 << bit]
        src = part.at[a, 0, strip(h)] if m == 0 else full.at[a, m, strip(h)]
        return copy(src, full.at[a, m | 1 << bit, strip(h)], s_ag.at[a, at], r_ag.at[a, at], partner(bit))

    arrived = set()

    def take(a, h, m):
        if m and (a, h, m) not in arrived:
            arrived.add((a, h, m))
            spread_copy(a, *source[h, m]).wait_recv()

    def relay(a):
        for h, bit, m in relayed:
            take(a, h, m)
            spread_copy(a, h, bit, m).start()

    tile = 256 if depth % 256 == 0 else 64
    masks = sorted(range(n), key=lambda v: bin(v).count("1"))

    def add_power(a, m):
        for h in range(2):
            take(a, h, m)
        held = part[a, 0] if m == 0 else full[a, m]
        inner[a, m] = held.astype(BF16)
        for at in range(0, depth, tile):
            rows = slice(at, at + tile)
            term = dot_t(inner[a, m], g_ref[m, rows, :])
            if m:
                term = rough[a, :, rows] + term
            if m == masks[-1]:
                power[a * half : (a + 1) * half, rows] = term.astype(BF16)
            else:
                rough[a, :, rows] = term

    grams = [(gram_a, gram_a_land), (gram_b, gram_b_land)]

    def gram_copy(a, phase, h):
        held, landed = grams[a]
        extent = held.shape[1] // 2
        rows = pl.ds(h * extent, extent)
        return copy(
            held.at[phase, rows], landed.at[phase, rows],
            s_gr.at[a, phase, h], r_gr.at[a, phase, h], partner(orders[h][phase]),
        )

    def gram_send(a, phase):
        for h in range(2):
            gram_copy(a, phase, h).start()

    def gram_add(a, phase):
        held, landed = grams[a]
        extent = held.shape[1] // 2
        for h in range(2):
            rows = slice(h * extent, (h + 1) * extent)
            gram_copy(a, phase, h).wait_recv()
            held[phase + 1, rows] = held[phase, rows] + landed[phase, rows]

    def total_copy(at):
        return copy(total.at[at], total_land.at[at], s_tot.at[at], r_tot.at[at], rounds[at][1])

    def total_start(at):
        if at == len(rounds):
            return
        if rounds[at][0] == SWAP:
            total_copy(at).start()
        else:
            pl.when(inside)(lambda: total_copy(at).start())

    def total_next(at):
        if at >= len(rounds):
            return
        kind = rounds[at][0]

        def add():
            total_copy(at).wait()
            total[at + 1] = total[at] + total_land[at]

        def give():
            total_copy(at).wait_send()
            total[at + 1] = total[at]

        def accept():
            total_copy(at).wait_recv()
            total[at + 1] = total_land[at]

        if kind == SWAP:
            add()
        elif kind == ACROSS:
            pl.when(inside)(add)
        else:
            pl.when(inside)(give)
            pl.when(jnp.logical_not(inside))(accept)
        total_start(at + 1)

    wanted = [move[2] for move in schedule[0]] + list(range(n))
    wanted = sorted(range(n), key=wanted.index)
    load_basis(0).start()
    load(wanted[0]).start()
    span = 128 if depth % 128 == 0 else depth

    def turn_basis(a):
        for at in range(0, depth, span):
            bt[a * half : (a + 1) * half, at : at + span] = b_ref[at : at + span, a * half : (a + 1) * half].T

    load_basis(0).wait()
    load_basis(1).start()
    for m in wanted[1:]:
        load(m).start()
    turn_basis(0)
    pl.semaphore_wait(barrier, greetings)

    def inner_part(a, m):
        part[a, m] = dot(bt[a * half : (a + 1) * half, :], g_ref[m])

    opening = schedule[0][:2]
    rest = schedule[0][2:]
    for m in wanted:
        load(m).wait()
        if m == wanted[-1]:
            load_basis(1).wait()
            turn_basis(1)
            inner_part(1, wanted[0])
            first[1].send(opening)
        inner_part(0, m)
        first[0].send([move for move in schedule[0] if move[2] == m])
    for m in wanted[1:]:
        inner_part(1, m)
    live = loads[0] >= 1
    refresh = jnp.logical_and(live, flags[0] == 1)
    first[0].forward()
    first[1].send(rest)

    def squares_of(step, sums):
        rows = pl.ds(pl.multiple_of(step * 16, 16), 16)
        for m in range(n):
            piece = g_ref[m, rows, :].astype(F32)
            sums = sums + piece * piece
        return sums

    sums = lax.fori_loop(0, depth // 16, squares_of, jnp.zeros((16, block), F32))
    total_sq = jnp.where(live, jnp.sum(sums), 0.0)
    count = jnp.where(jnp.logical_and(live, me == 0), 1.0, 0.0)
    tile_row = lax.broadcasted_iota(jnp.int32, (8, 128), 0)
    total[0] = jnp.where(tile_row == 0, total_sq, jnp.where(tile_row == 1, count, 0.0))
    total_start(0)
    first[1].forward()
    total_next(0)
    first[0].finish()
    for item in own:
        spread_copy(0, *item).start()
    add_power(0, 0)
    total_next(1)
    first[1].finish()
    for item in own[:2]:
        spread_copy(1, *item).start()
    total_next(2)
    add_power(1, 0)
    relay(0)
    for item in own[2:]:
        spread_copy(1, *item).start()
    relay(1)
    total_next(3)
    for m in masks[1:]:
        add_power(0, m)
    gram_a[0] = dot_t(power[0:half, :], power[0:half, :])
    gram_send(0, 0)

    def cross_part(a):
        for m in wanted:
            part2[a, m] = dot(power[a * half : (a + 1) * half, :], g_ref[m])

    cross_part(0)
    second[0].send(opening)
    for m in masks[1:-1]:
        add_power(1, m)
    for phase in range(bits - 1):
        gram_add(0, phase)
        gram_send(0, phase + 1)
    add_power(1, masks[-1])
    total_next(4)
    gram_b[0] = dot_t(power[...], power[half:size, :])
    gram_send(1, 0)
    second[0].send(rest)
    cross_part(1)
    gram_add(0, bits - 1)
    panels = half // PANEL
    work[...] = gram_a[bits]
    panel_steps(work, 0, panels // 4)
    for phase in range(bits - 1):
        gram_add(1, phase)
        gram_send(1, phase + 1)
    second[0].forward()
    second[1].send(schedule[0])
    panel_steps(work, panels // 4, panels)

    def write_fresh(a, pieces):
        for at in range(0, depth, tile):
            rows = slice(at, at + tile)
            columns = slice(a * half, (a + 1) * half)
            left = power[0 : (a + 1) * half, rows].T
            value = dot(left, pieces[2]) + dot(left, pieces[1]) + dot(left, pieces[0])
            kept = jnp.where(live, b_ref[rows, columns].astype(F32), 0.0)
            fresh[rows, columns] = jnp.where(refresh, value, kept)

    inverse_a = lower_of(work)
    write_fresh(0, pieces_of(inverse_a.T, 3))
    second[0].finish()
    turned_a = dot(inverse_a, part2[0, 0], HIGHEST)
    gram_add(1, bits - 1)
    upper = dot(inverse_a, gram_b[bits, 0:half], HIGHEST)
    work[...] = gram_b[bits, half:size] - dot(upper.T, upper, HIGHEST)
    panel_steps(work, 0, panels * 3 // 8)
    second[1].forward()
    panel_steps(work, panels * 3 // 8, panels)
    inverse_b = lower_of(work)
    mixed = -dot(inverse_b, dot(upper.T, inverse_a, HIGHEST), HIGHEST)
    write_fresh(1, pieces_of(jnp.concatenate([mixed, inverse_b], axis=1).T, 3))
    partly = dot(mixed, part2[0, 0], HIGHEST)
    inverse_pair = jnp.concatenate(pieces_of(inverse_b, 2), axis=1)
    for at in range(5, len(rounds)):
        total_next(at)
    final = total[len(rounds)]
    norm = lax.rsqrt(final[0:1, 0:1] / (final[1:2, 0:1] * entries) + 1e-6)

    def write_rot(a, turned):
        value = jnp.where(refresh, turned, jnp.where(live, part[a, 0], 0.0)) * norm
        rot[a * half : (a + 1) * half, :] = value

    write_rot(0, turned_a)
    second[1].finish()
    top, low = pieces_of(part2[1, 0], 2)
    turned_b = dot(inverse_pair, jnp.concatenate([low, low], axis=0))
    turned_b = turned_b + dot(inverse_pair, jnp.concatenate([top, top], axis=0))
    write_rot(1, partly + turned_b)
    for a in range(2):
        first[a].drain()
        second[a].drain()
        for item in spread:
            spread_copy(a, *item).wait_send()
        for phase in range(bits):
            for h in range(2):
                gram_copy(a, phase, h).wait_send()


def write_out(fresh, rot, fresh_hbm, rot_hbm, fresh_sem, rot_sem):
    depth = fresh.shape[0]
    extent = depth // PARTS
    copies = [pltpu.make_async_copy(rot, rot_hbm.at[0], rot_sem.at[0])]
    for at in range(PARTS):
        rows = pl.ds(at * extent, extent)
        copies.append(pltpu.make_async_copy(fresh.at[rows], fresh_hbm.at[0, rows], fresh_sem.at[at]))
    for item in copies:
        item.start()
    for item in copies:
        item.wait()


def on_device(n, experts, grads, basis, loads, flags):
    _, depth, wide = grads.shape
    size = basis.shape[2]
    half = size // 2
    block = wide // n
    bits = n.bit_length() - 1
    rounds = bits + experts.bit_length() - 1 + (experts == 8)
    moves = 2 * (n - 1)
    anywhere = pl.BlockSpec(memory_space=pl.ANY)
    vmem = pl.BlockSpec(memory_space=pltpu.VMEM)
    chunk = (half // 2, block)
    dma = pltpu.SemaphoreType.DMA
    new_basis, rotated = pl.pallas_call(
        functools.partial(kernel, n, experts, float(depth * n * wide)),
        out_shape=(pltpu.VMEM((depth, size), F32), pltpu.VMEM((size, block), F32)),
        in_specs=[pl.BlockSpec(memory_space=pltpu.HBM)] * 2 + [pl.BlockSpec(memory_space=pltpu.SMEM)] * 2,
        out_specs=(vmem, vmem),
        scratch_shapes=[
            pltpu.VMEM((n, depth, block), BF16),
            pltpu.VMEM((depth, size), BF16),
            pltpu.VMEM((size, depth), BF16),
            pltpu.VMEM((2, n, half, block), F32),
            pltpu.VMEM((2, moves, *chunk), F32),
            pltpu.VMEM((2, n, half, block), F32),
            pltpu.VMEM((2, n, half, block), BF16),
            pltpu.VMEM((2, half, depth), F32),
            pltpu.VMEM((size, depth), BF16),
            pltpu.VMEM((2, n, half, block), F32),
            pltpu.VMEM((2, moves, *chunk), F32),
            pltpu.VMEM((bits + 1, half, half), F32),
            pltpu.VMEM((bits, half, half), F32),
            pltpu.VMEM((bits + 1, size, half), F32),
            pltpu.VMEM((bits, size, half), F32),
            pltpu.VMEM((half, half), F32),
            pltpu.VMEM((rounds + 1, 8, 128), F32),
            pltpu.VMEM((rounds, 8, 128), F32),
            dma((n,)), dma((2,)),
            dma((2, moves)), dma((2, moves)), dma((2, moves)), dma((2, moves)), dma((2, moves)), dma((2, moves)),
            dma((2, bits, 2)), dma((2, bits, 2)), dma((rounds,)), dma((rounds,)),
        ],
        compiler_params=pltpu.CompilerParams(
            collective_id=0, has_side_effects=True, vmem_limit_bytes=32 * 1024 * 1024
        ),
    )(*[pltpu.with_memory_space_constraint(x, pltpu.HBM) for x in (grads[0], basis[0])], loads, flags)
    return pl.pallas_call(
        write_out,
        out_shape=(
            jax.ShapeDtypeStruct((1, depth, size), F32),
            jax.ShapeDtypeStruct((1, size, block), F32),
        ),
        in_specs=[vmem] * 2,
        out_specs=(anywhere, anywhere),
        scratch_shapes=[dma((PARTS,)), dma((1,))],
        compiler_params=pltpu.CompilerParams(vmem_limit_bytes=16 * 1024 * 1024),
    )(new_basis, rotated)


def solution(mesh):
    placed = (P("expert", "row", None), P("expert", "row", None), P("expert"), P("expert"))
    return jax.shard_map(
        functools.partial(on_device, mesh.shape["row"], mesh.shape["expert"]),
        mesh=mesh,
        in_specs=placed,
        out_specs=(P("expert", "row", None), P("expert", None, "row")),
        check_vma=False,
    )
```

```python
import functools

import jax
import jax.numpy as jnp
from jax import lax
from jax.experimental import pallas as pl
from jax.experimental.pallas import tpu as pltpu
from jax.sharding import PartitionSpec as P

PANEL = 16
PARTS = 4
SWAP, ACROSS, OUTWARD = range(3)
HIGHEST = lax.Precision.HIGHEST
F32 = jnp.float32
BF16 = jnp.bfloat16


def dot(a, b, precision=None):
    return lax.dot_general(a, b, (((1,), (0,)), ((), ())), precision=precision, preferred_element_type=F32)


def dot_t(a, b, precision=None):
    return lax.dot_general(a, b, (((1,), (1,)), ((), ())), precision=precision, preferred_element_type=F32)


def pieces_of(x, count):
    pieces = []
    for _ in range(count):
        pieces.append(x.astype(BF16))
        x = x - pieces[-1].astype(F32)
    return pieces


def first_bit(mask, order):
    for phase, bit in enumerate(order):
        if mask >> bit & 1:
            return phase
    return len(order)


def panel_step(work, step):
    size = work.shape[0]
    panel = work[0:PANEL, :]
    rows = lax.broadcasted_iota(jnp.int32, (PANEL, 128), 0)
    lanes = lax.broadcasted_iota(jnp.int32, (PANEL, 128), 1)
    columns = [jnp.broadcast_to(panel[:, j : j + 1], (PANEL, 128)) for j in range(PANEL)]
    pieces = [panel[:, at : at + 128] for at in range(0, size, 128)]
    unit = (rows == lanes).astype(F32)
    root = jnp.zeros((PANEL, 128), F32)
    for j in range(PANEL):
        inverse_root = lax.rsqrt(columns[j][j : j + 1, :])
        root = jnp.where(rows == j, inverse_root, root)
        factor = jnp.where(rows > j, columns[j] * (inverse_root * inverse_root), 0.0)
        for k in range(j + 1, PANEL):
            columns[k] = columns[k] - factor * columns[k][j : j + 1, :]
        pieces = [piece - factor * piece[j : j + 1, :] for piece in pieces]
        unit = unit - factor * unit[j : j + 1, :]
    scaled = [root * piece for piece in pieces]
    full = jnp.concatenate([jnp.where(lanes < PANEL, root * unit, scaled[0])] + scaled[1:], axis=1)
    where = lax.broadcasted_iota(jnp.int32, (PANEL, size), 1)
    open_columns = jnp.logical_and(where >= PANEL, where < size - PANEL * step)
    left = jnp.where(open_columns, jnp.concatenate(scaled, axis=1), 0.0)
    update = dot(left.T, full, HIGHEST)
    body = work[PANEL:, :]
    ahead = lax.broadcasted_iota(jnp.int32, body.shape, 1) < PANEL
    rest = jnp.where(ahead, 0.0, body) - update[PANEL:, :]
    work[0 : size - PANEL, :] = pltpu.roll(rest, size - PANEL, 1)
    work[size - PANEL :, :] = pltpu.roll(full, size - PANEL, 1)


def pack(square):
    size = square.shape[0]
    q = size // 4
    lane = lax.broadcasted_iota(jnp.int32, (q, size), 1)
    second = jnp.where(lane < q, pltpu.roll(square[3 * q :], q, 1), square[q : 2 * q])
    third = square[2 * q : 3 * q]
    lane = lane[: q // 2]
    third = jnp.where(lane < 2 * q, pltpu.roll(third[q // 2 :], 2 * q, 1), third[: q // 2])
    return jnp.concatenate([square[:q], second, third], axis=0)


def unpack(packed):
    size = packed.shape[1]
    q = size // 4
    second, third = packed[q : 2 * q], packed[2 * q :]
    rows = [packed[:q], second, third, pltpu.roll(third, 2 * q, 1), pltpu.roll(second, size - q, 1)]
    return jnp.concatenate(rows, axis=0)


def panel_steps(work, begin, end):
    def body(step, carry):
        panel_step(work, step)
        return carry

    lax.fori_loop(begin, end, body, 0)


def lower_of(work):
    shape = work.shape
    below = lax.broadcasted_iota(jnp.int32, shape, 1) <= lax.broadcasted_iota(jnp.int32, shape, 0)
    return jnp.where(below, work[...], 0.0)


def kernel(
    n, experts, entries, g_hbm, b_hbm, loads, flags, fresh, rot,
    g_ref, b_ref, bt, part, land, full, inner, rough, power, part2, land2,
    gram_a, gram_a_land, gram_b, gram_b_land, work, total, total_land,
    g_sem, b_sem,
    s_rs, r_rs, s_ag, r_ag, s_rs2, r_rs2, r_cut, s_gr, r_gr, s_tot, r_tot,
):
    _, depth, block = g_ref.shape
    bits = n.bit_length() - 1
    expert_bits = experts.bit_length() - 1
    size = b_ref.shape[1]
    half = size // 2
    sub = half // 2
    me = lax.axis_index("row")
    my_expert = lax.axis_index("expert")
    orders = [tuple(range(bits)), tuple(reversed(range(bits)))]
    cuts = g_sem.shape[1]

    def other(index, mask):
        at = index
        for bit in range(max(bits, expert_bits)):
            if mask >> bit & 1:
                at = at + (1 - 2 * (lax.rem(index // (1 << bit), 2))) * (1 << bit)
        return at

    def partner(bit):
        return {"row": other(me, 1 << bit), "expert": my_expert}

    def expert_partner(bit):
        return {"row": me, "expert": other(my_expert, 1 << bit)}

    place = my_expert // 2
    inside = jnp.logical_or(place == 1, place == 2)
    across = {"row": me, "expert": my_expert + jnp.where(place == 1, 2, -2)}
    if expert_bits == 3:
        rounds = [(SWAP, expert_partner(0)), (SWAP, expert_partner(1)), (ACROSS, across), (OUTWARD, expert_partner(1))]
    else:
        rounds = [(SWAP, expert_partner(b)) for b in range(expert_bits)]
    rounds = rounds + [(SWAP, partner(b)) for b in range(bits)]
    barrier = pltpu.get_barrier_semaphore()

    def greet(peer):
        pl.semaphore_signal(barrier, inc=1, device_id=peer, device_id_type=pl.DeviceIdType.MESH)

    greetings = 0
    for kind, peer in rounds:
        if kind == SWAP:
            greet(peer)
            greetings += 1
    if expert_bits == 3:
        pl.when(inside)(lambda: greet(across))
        greetings = greetings + inside.astype(jnp.int32)

    def load(m, cut):
        width = block // cuts
        columns = pl.ds(pl.multiple_of(other(me, m) * block + cut * width, width), width)
        return pltpu.make_async_copy(g_hbm.at[:, columns], g_ref.at[m, :, pl.ds(cut * width, width)], g_sem.at[m, cut])

    def load_basis(a):
        columns = pl.ds(a * half, half)
        return pltpu.make_async_copy(b_hbm.at[:, columns], b_ref.at[:, columns], b_sem.at[a])

    def copy(src, dst, send, recv, to):
        return pltpu.make_async_remote_copy(
            src_ref=src, dst_ref=dst, send_sem=send, recv_sem=recv,
            device_id=to, device_id_type=pl.DeviceIdType.MESH,
        )

    def settle(sent, sem):
        pltpu.make_async_copy(sent, sent, sem).wait()

    def strip(h):
        return pl.ds(h * sub, sub)

    schedule = []
    for phase in range(bits):
        lanes = []
        for h in range(2):
            order = orders[h]
            masks = [m for m in range(n) if first_bit(m, order) == phase]
            masks.sort(key=lambda m: first_bit(m & ~(1 << order[phase]), order))
            lanes.append([(h, phase, m, m & ~(1 << order[phase])) for m in masks])
        schedule.append([move for pair in zip(*lanes) for move in pair])
    slot = {}
    for phase_moves in schedule:
        for h, phase, m, there in phase_moves:
            slot[h, phase, there] = len(slot)

    class Halving:
        def __init__(self, a, parts, lands, sends, recvs, early):
            self.a, self.parts, self.lands, self.sends, self.recvs = a, parts, lands, sends, recvs
            self.early = early

        def make(self, h, phase, m, there):
            at = slot[h, phase, there]
            count = cuts if self.early and (h, phase, m, there) in schedule[0][:2] else 1
            width = block // count
            return [
                copy(
                    self.parts.at[self.a, m, strip(h), pl.ds(cut * width, width)],
                    self.lands.at[self.a, at, :, pl.ds(cut * width, width)],
                    self.sends.at[self.a], self.recvs.at[self.a, at] if cut == 0 else r_cut.at[h], partner(orders[h][phase]),
                )
                for cut in range(count)
            ]

        def absorb(self, h, phase, m):
            for item in self.make(h, phase, m | 1 << orders[h][phase], m):
                item.wait_recv()
            rows = slice(h * sub, (h + 1) * sub)
            self.parts[self.a, m, rows] = self.parts[self.a, m, rows] + self.lands[self.a, slot[h, phase, m]]

        def send(self, moves):
            for move in moves:
                for item in self.make(*move):
                    item.start()

        def forward(self):
            for phase in range(1, bits):
                for move in schedule[phase]:
                    for earlier in range(phase):
                        self.absorb(move[0], earlier, move[2])
                    self.send([move])

        def finish(self):
            for phase in range(bits):
                for h in range(2):
                    self.absorb(h, phase, 0)

        def drain(self):
            settle(self.parts.at[self.a, pl.ds(0, n - 1)], self.sends.at[self.a])

    first = [Halving(a, part, land, s_rs, r_rs, a == 0) for a in range(2)]
    second = [Halving(a, part2, land2, s_rs2, r_rs2, False) for a in range(2)]

    spread = []
    for h in range(2):
        held = [0]
        for bit in reversed(orders[h]):
            for m in list(held):
                spread.append((h, bit, m))
                held.append(m | 1 << bit)
    number = {(h, m | 1 << bit): at for at, (h, bit, m) in enumerate(spread)}
    source = {(h, m | 1 << bit): (h, bit, m) for h, bit, m in spread}
    own = [item for pair in zip(*[[s for s in spread if s[0] == h and s[2] == 0] for h in range(2)]) for item in pair]
    relayed = sorted((s for s in spread if s[2]), key=lambda s: bin(s[2]).count("1"))

    def spread_copy(a, h, bit, m):
        at = number[h, m | 1 << bit]
        src = part.at[a, 0, strip(h)] if m == 0 else full.at[a, m, strip(h)]
        return copy(src, full.at[a, m | 1 << bit, strip(h)], s_ag.at[a], r_ag.at[a, at], partner(bit))

    arrived = set()

    def take(a, h, m):
        if m and (a, h, m) not in arrived:
            arrived.add((a, h, m))
            spread_copy(a, *source[h, m]).wait_recv()

    def relay(a):
        for h, bit, m in relayed:
            take(a, h, m)
            spread_copy(a, h, bit, m).start()

    tile = 256 if depth % 256 == 0 else 64
    masks = sorted(range(n), key=lambda v: bin(v).count("1"))

    def add_power(a, m):
        for h in range(2):
            take(a, h, m)
        held = part[a, 0] if m == 0 else full[a, m]
        inner[a, m] = held.astype(BF16)
        for at in range(0, depth, tile):
            rows = slice(at, at + tile)
            term = dot_t(inner[a, m], g_ref[m, rows, :])
            if m:
                term = rough[a, :, rows] + term
            if m == masks[-1]:
                power[a * half : (a + 1) * half, rows] = term.astype(BF16)
            else:
                rough[a, :, rows] = term

    grams = [(gram_a, gram_a_land), (gram_b, gram_b_land)]

    def gram_copy(a, phase, h):
        held, landed = grams[a]
        extent = held.shape[1] // 2
        rows = pl.ds(h * extent, extent)
        return copy(
            held.at[phase, rows], landed.at[phase, rows],
            s_gr.at[a], r_gr.at[a, phase, h], partner(orders[h][phase]),
        )

    def gram_send(a, phase):
        for h in range(2):
            gram_copy(a, phase, h).start()

    def gram_add(a, phase):
        held, landed = grams[a]
        extent = held.shape[1] // 2
        for h in range(2):
            rows = slice(h * extent, (h + 1) * extent)
            gram_copy(a, phase, h).wait_recv()
            held[phase + 1, rows] = held[phase, rows] + landed[phase, rows]

    def total_copy(at):
        return copy(total.at[at], total_land.at[at], s_tot.at[0], r_tot.at[at], rounds[at][1])

    def total_start(at):
        if at == len(rounds):
            return
        if rounds[at][0] == SWAP:
            total_copy(at).start()
        else:
            pl.when(inside)(lambda: total_copy(at).start())

    def total_next(at):
        if at >= len(rounds):
            return
        kind = rounds[at][0]

        def add():
            total_copy(at).wait()
            total[at + 1] = total[at] + total_land[at]

        def give():
            total_copy(at).wait_send()
            total[at + 1] = total[at]

        def accept():
            total_copy(at).wait_recv()
            total[at + 1] = total_land[at]

        if kind == SWAP:
            add()
        elif kind == ACROSS:
            pl.when(inside)(add)
        else:
            pl.when(inside)(give)
            pl.when(jnp.logical_not(inside))(accept)
        total_start(at + 1)

    wanted = [move[2] for move in schedule[0]] + list(range(n))
    wanted = sorted(range(n), key=wanted.index)
    load_basis(0).start()
    for cut in range(cuts):
        load(wanted[0], cut).start()
    span = 128 if depth % 128 == 0 else depth

    def turn_basis(a):
        for at in range(0, depth, span):
            bt[a * half : (a + 1) * half, at : at + span] = b_ref[at : at + span, a * half : (a + 1) * half].T

    load_basis(0).wait()
    load_basis(1).start()
    for m in wanted[1:]:
        for cut in range(cuts):
            load(m, cut).start()
    turn_basis(0)
    pl.semaphore_wait(barrier, greetings)

    def inner_part(a, m):
        part[a, m] = dot(bt[a * half : (a + 1) * half, :], g_ref[m])

    opening = schedule[0][:2]
    rest = schedule[0][2:]
    for cut in range(cuts):
        load(wanted[0], cut).wait()
        columns = slice(cut * (block // cuts), (cut + 1) * (block // cuts))
        part[0, wanted[0], :, columns] = dot(bt[:half, :], g_ref[wanted[0], :, columns])
        for move in opening:
            first[0].make(*move)[cut].start()
    for m in wanted[1:]:
        for cut in range(cuts):
            load(m, cut).wait()
        if m == wanted[-1]:
            load_basis(1).wait()
            turn_basis(1)
            inner_part(1, wanted[0])
            first[1].send(opening)
        inner_part(0, m)
        first[0].send([move for move in rest if move[2] == m])
    for m in wanted[1:]:
        inner_part(1, m)
    live = loads[0] >= 1
    refresh = jnp.logical_and(live, flags[0] == 1)
    first[0].forward()
    first[1].send(rest)

    def squares_of(step, sums):
        rows = pl.ds(pl.multiple_of(step * 16, 16), 16)
        for m in range(n):
            piece = g_ref[m, rows, :].astype(F32)
            sums = sums + piece * piece
        return sums

    sums = lax.fori_loop(0, depth // 16, squares_of, jnp.zeros((16, block), F32))
    total_sq = jnp.where(live, jnp.sum(sums), 0.0)
    count = jnp.where(jnp.logical_and(live, me == 0), 1.0, 0.0)
    tile_row = lax.broadcasted_iota(jnp.int32, (8, 128), 0)
    total[0] = jnp.where(tile_row == 0, total_sq, jnp.where(tile_row == 1, count, 0.0))
    total_start(0)
    first[1].forward()
    total_next(0)
    first[0].finish()
    for item in own:
        spread_copy(0, *item).start()
    add_power(0, 0)
    total_next(1)
    first[1].finish()
    for item in own[:2]:
        spread_copy(1, *item).start()
    total_next(2)
    add_power(1, 0)
    relay(0)
    for item in own[2:]:
        spread_copy(1, *item).start()
    relay(1)
    total_next(3)
    for m in masks[1:]:
        add_power(0, m)
    gram_a[0] = pack(dot_t(power[0:half, :], power[0:half, :]))
    gram_send(0, 0)

    def cross_part(a):
        for m in wanted:
            part2[a, m] = dot(power[a * half : (a + 1) * half, :], g_ref[m])

    cross_part(0)
    second[0].send(opening)
    for m in masks[1:-1]:
        add_power(1, m)
    for phase in range(bits - 1):
        gram_add(0, phase)
        gram_send(0, phase + 1)
    add_power(1, masks[-1])
    total_next(4)
    both = dot_t(power[...], power[half:size, :])
    gram_b[0] = jnp.concatenate([both[:half], pack(both[half:])], axis=0)
    gram_send(1, 0)
    second[0].send(rest)
    cross_part(1)
    gram_add(0, bits - 1)
    panels = half // PANEL
    work[...] = unpack(gram_a[bits])
    panel_steps(work, 0, panels // 4)
    for phase in range(bits - 1):
        gram_add(1, phase)
        gram_send(1, phase + 1)
    second[0].forward()
    second[1].send(schedule[0])
    panel_steps(work, panels // 4, panels)

    def write_fresh(a, pieces):
        for at in range(0, depth, tile):
            rows = slice(at, at + tile)
            columns = slice(a * half, (a + 1) * half)
            left = power[0 : (a + 1) * half, rows].T
            value = dot(left, pieces[2]) + dot(left, pieces[1]) + dot(left, pieces[0])
            kept = jnp.where(live, b_ref[rows, columns].astype(F32), 0.0)
            fresh[rows, columns] = jnp.where(refresh, value, kept)

    inverse_a = lower_of(work)
    write_fresh(0, pieces_of(inverse_a.T, 3))
    gram_add(1, bits - 1)
    upper = dot(inverse_a, gram_b[bits, :half], HIGHEST)
    work[...] = unpack(gram_b[bits, half:]) - dot(upper.T, upper, HIGHEST)
    panel_steps(work, 0, panels * 3 // 4)
    second[0].finish()
    turned_a = dot(inverse_a, part2[0, 0], HIGHEST)
    second[1].forward()
    panel_steps(work, panels * 3 // 4, panels)
    inverse_b = lower_of(work)
    mixed = -dot(inverse_b, dot(upper.T, inverse_a, HIGHEST), HIGHEST)
    write_fresh(1, pieces_of(jnp.concatenate([mixed, inverse_b], axis=1).T, 3))
    partly = dot(mixed, part2[0, 0], HIGHEST)
    inverse_pair = jnp.concatenate(pieces_of(inverse_b, 2), axis=1)
    for at in range(5, len(rounds)):
        total_next(at)
    final = total[len(rounds)]
    norm = lax.rsqrt(final[0:1, 0:1] / (final[1:2, 0:1] * entries) + 1e-6)

    def write_rot(a, turned):
        value = jnp.where(refresh, turned, jnp.where(live, part[a, 0], 0.0)) * norm
        rot[a * half : (a + 1) * half, :] = value

    write_rot(0, turned_a)
    second[1].finish()
    top, low = pieces_of(part2[1, 0], 2)
    turned_b = dot(inverse_pair, jnp.concatenate([low, low], axis=0))
    turned_b = turned_b + dot(inverse_pair, jnp.concatenate([top, top], axis=0))
    write_rot(1, partly + turned_b)
    for a in range(2):
        first[a].drain()
        second[a].drain()
        settle(full.at[a, pl.ds(0, n - 1)], s_ag.at[a])
        settle(grams[a][0].at[pl.ds(0, bits)], s_gr.at[a])


def write_out(fresh, rot, fresh_hbm, rot_hbm, fresh_sem, rot_sem):
    depth = fresh.shape[0]
    extent = depth // PARTS
    copies = [pltpu.make_async_copy(rot, rot_hbm.at[0], rot_sem.at[0])]
    for at in range(PARTS):
        rows = pl.ds(at * extent, extent)
        copies.append(pltpu.make_async_copy(fresh.at[rows], fresh_hbm.at[0, rows], fresh_sem.at[at]))
    for item in copies:
        item.start()
    for item in copies:
        item.wait()


def on_device(n, experts, grads, basis, loads, flags):
    _, depth, wide = grads.shape
    size = basis.shape[2]
    half = size // 2
    block = wide // n
    bits = n.bit_length() - 1
    rounds = bits + experts.bit_length() - 1 + (experts == 8)
    moves = 2 * (n - 1)
    packed = half * 5 // 8
    cuts = 2 if block % 256 == 0 else 1
    anywhere = pl.BlockSpec(memory_space=pl.ANY)
    vmem = pl.BlockSpec(memory_space=pltpu.VMEM)
    chunk = (half // 2, block)
    dma = pltpu.SemaphoreType.DMA
    new_basis, rotated = pl.pallas_call(
        functools.partial(kernel, n, experts, float(depth * n * wide)),
        out_shape=(pltpu.VMEM((depth, size), F32), pltpu.VMEM((size, block), F32)),
        in_specs=[pl.BlockSpec(memory_space=pltpu.HBM)] * 2 + [pl.BlockSpec(memory_space=pltpu.SMEM)] * 2,
        out_specs=(vmem, vmem),
        scratch_shapes=[
            pltpu.VMEM((n, depth, block), BF16),
            pltpu.VMEM((depth, size), BF16),
            pltpu.VMEM((size, depth), BF16),
            pltpu.VMEM((2, n, half, block), F32),
            pltpu.VMEM((2, moves, *chunk), F32),
            pltpu.VMEM((2, n, half, block), F32),
            pltpu.VMEM((2, n, half, block), BF16),
            pltpu.VMEM((2, half, depth), F32),
            pltpu.VMEM((size, depth), BF16),
            pltpu.VMEM((2, n, half, block), F32),
            pltpu.VMEM((2, moves, *chunk), F32),
            pltpu.VMEM((bits + 1, packed, half), F32),
            pltpu.VMEM((bits, packed, half), F32),
            pltpu.VMEM((bits + 1, half + packed, half), F32),
            pltpu.VMEM((bits, half + packed, half), F32),
            pltpu.VMEM((half, half), F32),
            pltpu.VMEM((rounds + 1, 8, 128), F32),
            pltpu.VMEM((rounds, 8, 128), F32),
            dma((n, cuts)), dma((2,)),
            dma((2,)), dma((2, moves)), dma((2,)), dma((2, moves)), dma((2,)), dma((2, moves)), dma((2,)),
            dma((2,)), dma((2, bits, 2)), dma((1,)), dma((rounds,)),
        ],
        compiler_params=pltpu.CompilerParams(
            collective_id=0, has_side_effects=True, vmem_limit_bytes=32 * 1024 * 1024
        ),
    )(*[pltpu.with_memory_space_constraint(x, pltpu.HBM) for x in (grads[0], basis[0])], loads, flags)
    return pl.pallas_call(
        write_out,
        out_shape=(
            jax.ShapeDtypeStruct((1, depth, size), F32),
            jax.ShapeDtypeStruct((1, size, block), F32),
        ),
        in_specs=[vmem] * 2,
        out_specs=(anywhere, anywhere),
        scratch_shapes=[dma((PARTS,)), dma((1,))],
        compiler_params=pltpu.CompilerParams(vmem_limit_bytes=16 * 1024 * 1024),
    )(new_basis, rotated)


def solution(mesh):
    placed = (P("expert", "row", None), P("expert", "row", None), P("expert"), P("expert"))
    return jax.shard_map(
        functools.partial(on_device, mesh.shape["row"], mesh.shape["expert"]),
        mesh=mesh,
        in_specs=placed,
        out_specs=(P("expert", "row", None), P("expert", None, "row")),
        check_vma=False,
    )
```

```python
import functools

import jax
import jax.numpy as jnp
from jax import lax
from jax.experimental import pallas as pl
from jax.experimental.pallas import tpu as pltpu
from jax.sharding import PartitionSpec as P

PANEL = 16
PARTS = 4
SWAP, ACROSS, OUTWARD = range(3)
HIGHEST = lax.Precision.HIGHEST
F32 = jnp.float32
BF16 = jnp.bfloat16


def dot(a, b, precision=None):
    return lax.dot_general(a, b, (((1,), (0,)), ((), ())), precision=precision, preferred_element_type=F32)


def dot_t(a, b, precision=None):
    return lax.dot_general(a, b, (((1,), (1,)), ((), ())), precision=precision, preferred_element_type=F32)


def pieces_of(x, count):
    pieces = []
    for _ in range(count):
        pieces.append(x.astype(BF16))
        x = x - pieces[-1].astype(F32)
    return pieces


def scale_of(peak):
    scale = jnp.where(peak > 2.0**10, 2.0**-40, jnp.where(peak < 2.0**-10, 2.0**40, 1.0))
    return jnp.where(peak > 2.0**35, 2.0**-80, jnp.where(peak < 2.0**-35, 2.0**80, scale))


def first_bit(mask, order):
    for phase, bit in enumerate(order):
        if mask >> bit & 1:
            return phase
    return len(order)


def panel_step(work, step):
    size = work.shape[0]
    panel = work[0:PANEL, :]
    rows = lax.broadcasted_iota(jnp.int32, (PANEL, 128), 0)
    lanes = lax.broadcasted_iota(jnp.int32, (PANEL, 128), 1)
    columns = [jnp.broadcast_to(panel[:, j : j + 1], (PANEL, 128)) for j in range(PANEL)]
    pieces = [panel[:, at : at + 128] for at in range(0, size, 128)]
    unit = (rows == lanes).astype(F32)
    root = jnp.zeros((PANEL, 128), F32)
    for j in range(PANEL):
        inverse_root = lax.rsqrt(columns[j][j : j + 1, :])
        root = jnp.where(rows == j, inverse_root, root)
        factor = jnp.where(rows > j, columns[j] * (inverse_root * inverse_root), 0.0)
        for k in range(j + 1, PANEL):
            columns[k] = columns[k] - factor * columns[k][j : j + 1, :]
        pieces = [piece - factor * piece[j : j + 1, :] for piece in pieces]
        unit = unit - factor * unit[j : j + 1, :]
    scaled = [root * piece for piece in pieces]
    full = jnp.concatenate([jnp.where(lanes < PANEL, root * unit, scaled[0])] + scaled[1:], axis=1)
    where = lax.broadcasted_iota(jnp.int32, (PANEL, size), 1)
    open_columns = jnp.logical_and(where >= PANEL, where < size - PANEL * step)
    left = jnp.where(open_columns, jnp.concatenate(scaled, axis=1), 0.0)
    update = dot(left.T, full, HIGHEST)
    body = work[PANEL:, :]
    ahead = lax.broadcasted_iota(jnp.int32, body.shape, 1) < PANEL
    rest = jnp.where(ahead, 0.0, body) - update[PANEL:, :]
    work[0 : size - PANEL, :] = pltpu.roll(rest, size - PANEL, 1)
    work[size - PANEL :, :] = pltpu.roll(full, size - PANEL, 1)


def pack(square):
    size = square.shape[0]
    q = size // 4
    lane = lax.broadcasted_iota(jnp.int32, (q, size), 1)
    second = jnp.where(lane < q, pltpu.roll(square[3 * q :], q, 1), square[q : 2 * q])
    third = square[2 * q : 3 * q]
    lane = lane[: q // 2]
    third = jnp.where(lane < 2 * q, pltpu.roll(third[q // 2 :], 2 * q, 1), third[: q // 2])
    return jnp.concatenate([square[:q], second, third], axis=0)


def unpack(packed):
    size = packed.shape[1]
    q = size // 4
    second, third = packed[q : 2 * q], packed[2 * q :]
    rows = [packed[:q], second, third, pltpu.roll(third, 2 * q, 1), pltpu.roll(second, size - q, 1)]
    return jnp.concatenate(rows, axis=0)


def panel_steps(work, begin, end):
    def body(step, carry):
        panel_step(work, step)
        return carry

    lax.fori_loop(begin, end, body, 0)


def lower_of(work):
    shape = work.shape
    below = lax.broadcasted_iota(jnp.int32, shape, 1) <= lax.broadcasted_iota(jnp.int32, shape, 0)
    return jnp.where(below, work[...], 0.0)


def kernel(
    n, experts, entries, g_hbm, b_hbm, loads, flags, fresh, rot, pair, cross,
    g_ref, b_ref, bt, part, land, full, inner, rough, power, part2, land2,
    gram_a, gram_a_land, gram_b, gram_b_land, work, total, total_land,
    g_sem, b_sem,
    s_rs, r_rs, s_ag, r_ag, s_rs2, r_rs2, s_gr, r_gr, s_tot, r_tot,
):
    _, depth, block = g_ref.shape
    bits = n.bit_length() - 1
    expert_bits = experts.bit_length() - 1
    size = b_ref.shape[1]
    half = size // 2
    sub = half // 2
    me = lax.axis_index("row")
    my_expert = lax.axis_index("expert")
    orders = [tuple(range(bits)), tuple(reversed(range(bits)))]
    cuts = g_sem.shape[0] - n + 1

    def other(index, mask):
        at = index
        for bit in range(max(bits, expert_bits)):
            if mask >> bit & 1:
                at = at + (1 - 2 * (lax.rem(index // (1 << bit), 2))) * (1 << bit)
        return at

    def partner(bit):
        return {"row": other(me, 1 << bit), "expert": my_expert}

    def expert_partner(bit):
        return {"row": me, "expert": other(my_expert, 1 << bit)}

    place = my_expert // 2
    inside = jnp.logical_or(place == 1, place == 2)
    across = {"row": me, "expert": my_expert + jnp.where(place == 1, 2, -2)}
    if expert_bits == 3:
        rounds = [(SWAP, expert_partner(0)), (SWAP, expert_partner(1)), (ACROSS, across), (OUTWARD, expert_partner(1))]
    else:
        rounds = [(SWAP, expert_partner(b)) for b in range(expert_bits)]
    rounds = rounds + [(SWAP, partner(b)) for b in range(bits)]
    barrier = pltpu.get_barrier_semaphore()

    def greet(peer):
        pl.semaphore_signal(barrier, inc=1, device_id=peer, device_id_type=pl.DeviceIdType.MESH)

    greetings = 0
    for kind, peer in rounds:
        if kind == SWAP:
            greet(peer)
            greetings += 1
    if expert_bits == 3:
        pl.when(inside)(lambda: greet(across))
        greetings = greetings + inside.astype(jnp.int32)

    def load(index, cut=0):
        m = wanted[index]
        width = block if index else block // cuts
        columns = pl.ds(pl.multiple_of(other(me, m) * block + cut * width, width), width)
        sem = g_sem.at[cuts - 1 + index if index else cut]
        return pltpu.make_async_copy(g_hbm.at[:, columns], g_ref.at[m, :, pl.ds(cut * width, width)], sem)

    def load_basis(a):
        columns = pl.ds(a * half, half)
        return pltpu.make_async_copy(b_hbm.at[:, columns], b_ref.at[:, columns], b_sem.at[a])

    def copy(src, dst, send, recv, to):
        return pltpu.make_async_remote_copy(
            src_ref=src, dst_ref=dst, send_sem=send, recv_sem=recv,
            device_id=to, device_id_type=pl.DeviceIdType.MESH,
        )

    def settle(sent, sem):
        pltpu.make_async_copy(sent, sent, sem).wait()

    def strip(h):
        return pl.ds(h * sub, sub)

    schedule = []
    for phase in range(bits):
        lanes = []
        for h in range(2):
            order = orders[h]
            masks = [m for m in range(n) if first_bit(m, order) == phase]
            masks.sort(key=lambda m: first_bit(m & ~(1 << order[phase]), order))
            lanes.append([(h, phase, m, m & ~(1 << order[phase])) for m in masks])
        schedule.append([move for pair in zip(*lanes) for move in pair])
    slot = {}
    for phase_moves in schedule:
        for h, phase, m, there in phase_moves:
            slot[h, phase, there] = len(slot)

    def stage(h, m):
        return first_bit(m, orders[h]) % bits

    stages = [stage(h, there) for h, _, there in slot]

    class Halving:
        def __init__(self, a, parts, lands, sends, recvs, early):
            self.a, self.parts, self.lands, self.sends, self.recvs = a, parts, lands, sends, recvs
            self.early = early
            self.landed = set()

        def make(self, h, phase, m, there):
            at = slot[h, phase, there]
            count = cuts if self.early and (h, phase, m, there) in schedule[0][:2] else 1
            width = block // count
            return [
                copy(
                    self.parts.at[self.a, m, strip(h), pl.ds(cut * width, width)],
                    self.lands.at[self.a, at, :, pl.ds(cut * width, width)],
                    self.sends.at[self.a], self.recvs.at[self.a, stage(h, there)], partner(orders[h][phase]),
                )
                for cut in range(count)
            ]

        def absorb(self, h, phase, m):
            group = stage(h, m)
            if group not in self.landed:
                self.landed.add(group)
                settle(land.at[0, pl.ds(0, stages.count(group))], self.recvs.at[self.a, group])
            rows = slice(h * sub, (h + 1) * sub)
            self.parts[self.a, m, rows] = self.parts[self.a, m, rows] + self.lands[self.a, slot[h, phase, m]]

        def send(self, moves):
            for move in moves:
                for item in self.make(*move):
                    item.start()

        def forward(self):
            for phase in range(1, bits):
                for move in schedule[phase]:
                    for earlier in range(phase):
                        self.absorb(move[0], earlier, move[2])
                    self.send([move])

        def finish(self):
            for phase in range(bits):
                for h in range(2):
                    self.absorb(h, phase, 0)

        def drain(self):
            settle(self.parts.at[self.a, pl.ds(0, n - 1)], self.sends.at[self.a])

    first = [Halving(a, part, land, s_rs, r_rs, a == 0) for a in range(2)]
    second = [Halving(a, part2, land2, s_rs2, r_rs2, False) for a in range(2)]

    spread = []
    for h in range(2):
        held = [0]
        for bit in reversed(orders[h]):
            for m in list(held):
                spread.append((h, bit, m))
                held.append(m | 1 << bit)
    passed = {(h, m) for h, _, m in spread}
    groups = {}
    for h, bit, m in spread:
        there = m | 1 << bit
        level = bin(there).count("1")
        groups[h, there] = 2 * level - 2 + ((h, there) not in passed)
    names = sorted(set(groups.values()))
    groups = {key: names.index(value) for key, value in groups.items()}
    own = [item for pair in zip(*[[s for s in spread if s[0] == h and s[2] == 0] for h in range(2)]) for item in pair]
    relayed = sorted((s for s in spread if s[2]), key=lambda s: bin(s[2]).count("1"))

    def spread_copy(a, h, bit, m):
        src = part.at[a, 0, strip(h)] if m == 0 else full.at[a, m, strip(h)]
        return copy(src, full.at[a, m | 1 << bit, strip(h)], s_ag.at[a], r_ag.at[a, groups[h, m | 1 << bit]], partner(bit))

    arrived = set()

    def take(a, h, m):
        if m and (a, groups[h, m]) not in arrived:
            arrived.add((a, groups[h, m]))
            count = list(groups.values()).count(groups[h, m])
            settle(land.at[0, pl.ds(0, count)], r_ag.at[a, groups[h, m]])

    def relay(a):
        for h, bit, m in relayed:
            take(a, h, m)
            spread_copy(a, h, bit, m).start()

    tile = 256 if depth % 256 == 0 else 64
    masks = sorted(range(n), key=lambda v: bin(v).count("1"))

    largest = {}

    def add_power(a, m):
        for h in range(2):
            take(a, h, m)
        held = part[a, 0] if m == 0 else full[a, m]
        inner[a, m] = held.astype(BF16)
        peak = jnp.max(jnp.abs(held), axis=0, keepdims=True)
        largest[a] = peak if m == 0 else jnp.maximum(largest[a], peak)
        if m == masks[-1]:
            scale = scale_of(jnp.max(largest[a], axis=1, keepdims=True))
        for at in range(0, depth, tile):
            rows = slice(at, at + tile)
            term = dot_t(inner[a, m], g_ref[m, rows, :])
            if m:
                term = rough[a, :, rows] + term
            if m == masks[-1]:
                power[a * half : (a + 1) * half, rows] = (term * scale).astype(BF16)
            else:
                rough[a, :, rows] = term

    grams = [(gram_a, gram_a_land), (gram_b, gram_b_land)]

    def gram_copy(a, phase, h):
        held, landed = grams[a]
        extent = held.shape[1] // 2
        rows = pl.ds(h * extent, extent)
        return copy(
            held.at[phase, rows], landed.at[phase, rows],
            s_gr.at[a], r_gr.at[a, phase], partner(orders[h][phase]),
        )

    def gram_send(a, phase):
        for h in range(2):
            gram_copy(a, phase, h).start()

    def gram_add(a, phase):
        held, landed = grams[a]
        settle(landed.at[phase], r_gr.at[a, phase])
        held[phase + 1] = held[phase] + landed[phase]

    def total_copy(at):
        return copy(total.at[at], total_land.at[at], s_tot.at[0], r_tot.at[at], rounds[at][1])

    def total_start(at):
        if at == len(rounds):
            return
        if rounds[at][0] == SWAP:
            total_copy(at).start()
        else:
            pl.when(inside)(lambda: total_copy(at).start())

    def total_next(at):
        if at >= len(rounds):
            return
        kind = rounds[at][0]

        def add():
            total_copy(at).wait()
            total[at + 1] = total[at] + total_land[at]

        def give():
            total_copy(at).wait_send()
            total[at + 1] = total[at]

        def accept():
            total_copy(at).wait_recv()
            total[at + 1] = total_land[at]

        if kind == SWAP:
            add()
        elif kind == ACROSS:
            pl.when(inside)(add)
        else:
            pl.when(inside)(give)
            pl.when(jnp.logical_not(inside))(accept)
        total_start(at + 1)

    wanted = [move[2] for move in schedule[0]] + list(range(n))
    wanted = sorted(range(n), key=wanted.index)
    load_basis(0).start()
    for cut in range(cuts):
        load(0, cut).start()
    span = 128 if depth % 128 == 0 else depth

    def turn_basis(a):
        for at in range(0, depth, span):
            bt[a * half : (a + 1) * half, at : at + span] = b_ref[at : at + span, a * half : (a + 1) * half].T

    load_basis(0).wait()
    for index in range(1, n):
        load(index).start()
    load_basis(1).start()
    turn_basis(0)

    def inner_part(a, m):
        part[a, m] = dot(bt[a * half : (a + 1) * half, :], g_ref[m])

    opening = schedule[0][:2]
    rest = schedule[0][2:]
    for cut in range(cuts):
        load(0, cut).wait()
        columns = slice(cut * (block // cuts), (cut + 1) * (block // cuts))
        part[0, wanted[0], :, columns] = dot(bt[:half, :], g_ref[wanted[0], :, columns])
        if cut == 0:
            pl.semaphore_wait(barrier, greetings)
        for move in opening:
            first[0].make(*move)[cut].start()
    for index in range(1, n):
        load(index).wait()
        m = wanted[index]
        if m == wanted[-1]:
            load_basis(1).wait()
            turn_basis(1)
            inner_part(1, wanted[0])
            first[1].send(opening)
        inner_part(0, m)
        first[0].send([move for move in rest if move[2] == m])
    for m in wanted[1:]:
        inner_part(1, m)
    live = loads[0] >= 1
    refresh = jnp.logical_and(live, flags[0] == 1)
    first[0].forward()
    first[1].send(rest)

    def squares_of(step, sums):
        rows = pl.ds(pl.multiple_of(step * 16, 16), 16)
        for m in range(n):
            piece = g_ref[m, rows, :].astype(F32)
            sums = sums + piece * piece
        return sums

    sums = lax.fori_loop(0, depth // 16, squares_of, jnp.zeros((16, block), F32))
    total_sq = jnp.where(live, jnp.sum(sums), 0.0)
    count = jnp.where(jnp.logical_and(live, me == 0), 1.0, 0.0)
    tile_row = lax.broadcasted_iota(jnp.int32, (8, 128), 0)
    total[0] = jnp.where(tile_row == 0, total_sq, jnp.where(tile_row == 1, count, 0.0))
    total_start(0)
    first[1].forward()
    total_next(0)
    first[0].finish()
    for item in own:
        spread_copy(0, *item).start()
    add_power(0, 0)
    total_next(1)
    first[1].finish()
    for item in own[:2]:
        spread_copy(1, *item).start()
    total_next(2)
    add_power(1, 0)
    relay(0)
    for item in own[2:]:
        spread_copy(1, *item).start()
    relay(1)
    total_next(3)
    for m in masks[1:]:
        add_power(0, m)
    gram_a[0] = pack(dot_t(power[0:half, :], power[0:half, :]))
    gram_send(0, 0)

    def cross_part(a):
        for m in wanted:
            part2[a, m] = dot(power[a * half : (a + 1) * half, :], g_ref[m])

    cross_part(0)
    second[0].send(opening)
    for m in masks[1:-1]:
        add_power(1, m)
    for phase in range(bits - 1):
        gram_add(0, phase)
        gram_send(0, phase + 1)
    add_power(1, masks[-1])
    total_next(4)
    both = dot_t(power[...], power[half:size, :])
    gram_b[0] = jnp.concatenate([both[:half], pack(both[half:])], axis=0)
    gram_send(1, 0)
    second[0].send(rest)
    cross_part(1)
    gram_add(0, bits - 1)
    panels = half // PANEL
    work[...] = unpack(gram_a[bits])
    panel_steps(work, 0, panels // 4)
    for phase in range(bits - 1):
        gram_add(1, phase)
        gram_send(1, phase + 1)
    second[0].forward()
    second[1].send(schedule[0])
    panel_steps(work, panels // 4, panels)

    def write_fresh(a, pieces):
        for at in range(0, depth, tile):
            rows = slice(at, at + tile)
            columns = slice(a * half, (a + 1) * half)
            left = power[0 : (a + 1) * half, rows].T
            value = dot(left, pieces[2]) + dot(left, pieces[1]) + dot(left, pieces[0])
            kept = jnp.where(live, b_ref[rows, columns].astype(F32), 0.0)
            fresh[rows, columns] = jnp.where(refresh, value, kept)

    inverse_a = lower_of(work)
    write_fresh(0, pieces_of(inverse_a.T, 3))
    gram_add(1, bits - 1)
    upper = dot(inverse_a, gram_b[bits, :half], HIGHEST)
    work[...] = unpack(gram_b[bits, half:]) - dot(upper.T, upper, HIGHEST)
    panel_steps(work, 0, panels * 3 // 4)
    second[0].finish()
    turned_a = dot(inverse_a, part2[0, 0], HIGHEST)
    second[1].forward()
    panel_steps(work, panels * 3 // 4, panels)
    inverse_b = lower_of(work)
    mixed = -dot(inverse_b, dot(upper.T, inverse_a, HIGHEST), HIGHEST)
    write_fresh(1, pieces_of(jnp.concatenate([mixed, inverse_b], axis=1).T, 3))
    for at in range(5, len(rounds)):
        total_next(at)
    final = total[len(rounds)]
    norm = lax.rsqrt(final[0:1, 0:1] / (final[1:2, 0:1] * entries) + 1e-6)

    def write_rot(a, turned):
        rot[a * half : (a + 1) * half, :] = jnp.where(refresh, turned, jnp.where(live, part[a, 0], 0.0)) * norm

    write_rot(0, turned_a)
    write_rot(1, dot(mixed, part2[0, 0], HIGHEST))
    pair[...] = jnp.concatenate(pieces_of(jnp.where(refresh, inverse_b * norm, 0.0), 2), axis=1)
    second[1].finish()
    cross[...] = jnp.where(refresh, part2[1, 0], 0.0)
    for a in range(2):
        first[a].drain()
        second[a].drain()
        settle(full.at[a, pl.ds(0, n - 1)], s_ag.at[a])
        settle(grams[a][0].at[pl.ds(0, bits)], s_gr.at[a])


def write_out(fresh, rot, pair, cross, fresh_hbm, rot_hbm, last, fresh_sem, rot_sem):
    extent = fresh.shape[0] // PARTS
    half = cross.shape[0]
    copies = [pltpu.make_async_copy(rot.at[pl.ds(0, half)], rot_hbm.at[0, pl.ds(0, half)], rot_sem.at[0])]
    for at in range(PARTS):
        rows = pl.ds(at * extent, extent)
        copies.append(pltpu.make_async_copy(fresh.at[rows], fresh_hbm.at[0, rows], fresh_sem.at[at]))
    for item in copies:
        item.start()
    top, low = pieces_of(cross[...], 2)
    turned = dot(pair[...], jnp.concatenate([low, low], axis=0)) + dot(pair[...], jnp.concatenate([top, top], axis=0))
    last[...] = rot[half:, :] + turned
    copies.append(pltpu.make_async_copy(last, rot_hbm.at[0, pl.ds(half, half)], rot_sem.at[1]))
    copies[-1].start()
    for item in copies:
        item.wait()


def on_device(n, experts, grads, basis, loads, flags):
    _, depth, wide = grads.shape
    size = basis.shape[2]
    half = size // 2
    block = wide // n
    bits = n.bit_length() - 1
    rounds = bits + experts.bit_length() - 1 + (experts == 8)
    moves = 2 * (n - 1)
    packed = half * 5 // 8
    cuts = 2 if block % 256 == 0 else 1
    anywhere = pl.BlockSpec(memory_space=pl.ANY)
    vmem = pl.BlockSpec(memory_space=pltpu.VMEM)
    chunk = (half // 2, block)
    dma = pltpu.SemaphoreType.DMA
    results = pl.pallas_call(
        functools.partial(kernel, n, experts, float(depth * n * wide)),
        out_shape=(
            pltpu.VMEM((depth, size), F32), pltpu.VMEM((size, block), F32),
            pltpu.VMEM((half, size), BF16), pltpu.VMEM((half, block), F32),
        ),
        in_specs=[pl.BlockSpec(memory_space=pltpu.HBM)] * 2 + [pl.BlockSpec(memory_space=pltpu.SMEM)] * 2,
        out_specs=(vmem, vmem, vmem, vmem),
        scratch_shapes=[
            pltpu.VMEM((n, depth, block), BF16),
            pltpu.VMEM((depth, size), BF16),
            pltpu.VMEM((size, depth), BF16),
            pltpu.VMEM((2, n, half, block), F32),
            pltpu.VMEM((2, moves, *chunk), F32),
            pltpu.VMEM((2, n, half, block), F32),
            pltpu.VMEM((2, n, half, block), BF16),
            pltpu.VMEM((2, half, depth), F32),
            pltpu.VMEM((size, depth), BF16),
            pltpu.VMEM((2, n, half, block), F32),
            pltpu.VMEM((2, moves, *chunk), F32),
            pltpu.VMEM((bits + 1, packed, half), F32),
            pltpu.VMEM((bits, packed, half), F32),
            pltpu.VMEM((bits + 1, half + packed, half), F32),
            pltpu.VMEM((bits, half + packed, half), F32),
            pltpu.VMEM((half, half), F32),
            pltpu.VMEM((rounds + 1, 8, 128), F32),
            pltpu.VMEM((rounds, 8, 128), F32),
            dma((n - 1 + cuts,)), dma((2,)),
            dma((2,)), dma((2, bits)), dma((2,)), dma((2, 2 * bits - 1)), dma((2,)), dma((2, bits)),
            dma((2,)), dma((2, bits)), dma((1,)), dma((rounds,)),
        ],
        compiler_params=pltpu.CompilerParams(
            collective_id=0, has_side_effects=True, vmem_limit_bytes=32 * 1024 * 1024
        ),
    )(*[pltpu.with_memory_space_constraint(x, pltpu.HBM) for x in (grads[0], basis[0])], loads, flags)
    return pl.pallas_call(
        write_out,
        out_shape=(
            jax.ShapeDtypeStruct((1, depth, size), F32),
            jax.ShapeDtypeStruct((1, size, block), F32),
        ),
        in_specs=[vmem] * 4,
        out_specs=(anywhere, anywhere),
        scratch_shapes=[pltpu.VMEM((half, block), F32), dma((PARTS,)), dma((2,))],
        compiler_params=pltpu.CompilerParams(vmem_limit_bytes=16 * 1024 * 1024),
    )(*results)


def solution(mesh):
    placed = (P("expert", "row", None), P("expert", "row", None), P("expert"), P("expert"))
    return jax.shard_map(
        functools.partial(on_device, mesh.shape["row"], mesh.shape["expert"]),
        mesh=mesh,
        in_specs=placed,
        out_specs=(P("expert", "row", None), P("expert", None, "row")),
        check_vma=False,
    )
```

```python
import functools

import jax
import jax.numpy as jnp
from jax import lax
from jax.experimental import pallas as pl
from jax.experimental.pallas import tpu as pltpu
from jax.sharding import PartitionSpec as P

PANEL = 16
PARTS = 4
SWAP, ACROSS, OUTWARD = range(3)
HIGHEST = lax.Precision.HIGHEST
F32 = jnp.float32
BF16 = jnp.bfloat16


def dot(a, b, precision=None):
    return lax.dot_general(a, b, (((1,), (0,)), ((), ())), precision=precision, preferred_element_type=F32)


def dot_t(a, b, precision=None):
    return lax.dot_general(a, b, (((1,), (1,)), ((), ())), precision=precision, preferred_element_type=F32)


def pieces_of(x, count):
    pieces = []
    for _ in range(count):
        pieces.append(x.astype(BF16))
        x = x - pieces[-1].astype(F32)
    return pieces


def scale_of(peak):
    scale = jnp.where(peak > 2.0**10, 2.0**-40, jnp.where(peak < 2.0**-10, 2.0**40, 1.0))
    return jnp.where(peak > 2.0**35, 2.0**-80, jnp.where(peak < 2.0**-35, 2.0**80, scale))


def first_bit(mask, order):
    for phase, bit in enumerate(order):
        if mask >> bit & 1:
            return phase
    return len(order)


def panel_step(work, step):
    size = work.shape[0]
    panel = work[0:PANEL, :]
    rows = lax.broadcasted_iota(jnp.int32, (PANEL, 128), 0)
    lanes = lax.broadcasted_iota(jnp.int32, (PANEL, 128), 1)
    columns = [jnp.broadcast_to(panel[:, j : j + 1], (PANEL, 128)) for j in range(PANEL)]
    pieces = [panel[:, at : at + 128] for at in range(0, size, 128)]
    unit = (rows == lanes).astype(F32)
    root = jnp.zeros((PANEL, 128), F32)
    for j in range(PANEL):
        inverse_root = lax.rsqrt(columns[j][j : j + 1, :])
        root = jnp.where(rows == j, inverse_root, root)
        factor = jnp.where(rows > j, columns[j] * (inverse_root * inverse_root), 0.0)
        for k in range(j + 1, PANEL):
            columns[k] = columns[k] - factor * columns[k][j : j + 1, :]
        pieces = [piece - factor * piece[j : j + 1, :] for piece in pieces]
        unit = unit - factor * unit[j : j + 1, :]
    scaled = [root * piece for piece in pieces]
    full = jnp.concatenate([jnp.where(lanes < PANEL, root * unit, scaled[0])] + scaled[1:], axis=1)
    where = lax.broadcasted_iota(jnp.int32, (PANEL, size), 1)
    open_columns = jnp.logical_and(where >= PANEL, where < size - PANEL * step)
    left = jnp.where(open_columns, jnp.concatenate(scaled, axis=1), 0.0)
    update = dot(left.T, full, HIGHEST)
    body = work[PANEL:, :]
    ahead = lax.broadcasted_iota(jnp.int32, body.shape, 1) < PANEL
    rest = jnp.where(ahead, 0.0, body) - update[PANEL:, :]
    work[0 : size - PANEL, :] = pltpu.roll(rest, size - PANEL, 1)
    work[size - PANEL :, :] = pltpu.roll(full, size - PANEL, 1)


def pack(square):
    size = square.shape[0]
    q = size // 4
    lane = lax.broadcasted_iota(jnp.int32, (q, size), 1)
    second = jnp.where(lane < q, pltpu.roll(square[3 * q :], q, 1), square[q : 2 * q])
    third = square[2 * q : 3 * q]
    lane = lane[: q // 2]
    third = jnp.where(lane < 2 * q, pltpu.roll(third[q // 2 :], 2 * q, 1), third[: q // 2])
    return jnp.concatenate([square[:q], second, third], axis=0)


def unpack(packed):
    size = packed.shape[1]
    q = size // 4
    second, third = packed[q : 2 * q], packed[2 * q :]
    rows = [packed[:q], second, third, pltpu.roll(third, 2 * q, 1), pltpu.roll(second, size - q, 1)]
    return jnp.concatenate(rows, axis=0)


def panel_steps(work, begin, end):
    def body(step, carry):
        panel_step(work, step)
        return carry

    lax.fori_loop(begin, end, body, 0)


def lower_of(work):
    shape = work.shape
    below = lax.broadcasted_iota(jnp.int32, shape, 1) <= lax.broadcasted_iota(jnp.int32, shape, 0)
    return jnp.where(below, work[...], 0.0)


def kernel(
    n, experts, entries, g_hbm, b_hbm, loads, flags, fresh, rot, pair, cross,
    g_ref, b_ref, bt, part, land, full, inner, rough, power, part2, land2,
    gram_a, gram_a_land, gram_b, gram_b_land, work, total, total_land,
    g_sem, b_sem,
    s_rs, r_rs, s_ag, r_ag, s_rs2, r_rs2, s_gr, r_gr, s_tot, r_tot,
):
    _, depth, block = g_ref.shape
    bits = n.bit_length() - 1
    expert_bits = experts.bit_length() - 1
    size = b_ref.shape[1]
    half = size // 2
    sub = half // 2
    me = lax.axis_index("row")
    my_expert = lax.axis_index("expert")
    orders = [tuple(range(bits)), tuple(reversed(range(bits)))]
    cuts = g_sem.shape[0] - n + 1

    def other(index, mask):
        at = index
        for bit in range(max(bits, expert_bits)):
            if mask >> bit & 1:
                at = at + (1 - 2 * (lax.rem(index // (1 << bit), 2))) * (1 << bit)
        return at

    def partner(bit):
        return {"row": other(me, 1 << bit), "expert": my_expert}

    def expert_partner(bit):
        return {"row": me, "expert": other(my_expert, 1 << bit)}

    place = my_expert // 2
    inside = jnp.logical_or(place == 1, place == 2)
    across = {"row": me, "expert": my_expert + jnp.where(place == 1, 2, -2)}
    if expert_bits == 3:
        rounds = [(SWAP, expert_partner(0)), (SWAP, expert_partner(1)), (ACROSS, across), (OUTWARD, expert_partner(1))]
    else:
        rounds = [(SWAP, expert_partner(b)) for b in range(expert_bits)]
    rounds = rounds + [(SWAP, partner(b)) for b in range(bits)]
    barrier = pltpu.get_barrier_semaphore()

    def greet(peer):
        pl.semaphore_signal(barrier, inc=1, device_id=peer, device_id_type=pl.DeviceIdType.MESH)

    greetings = 0
    for kind, peer in rounds:
        if kind == SWAP:
            greet(peer)
            greetings += 1
    if expert_bits == 3:
        pl.when(inside)(lambda: greet(across))
        greetings = greetings + inside.astype(jnp.int32)

    def load(index, cut=0):
        m = wanted[index]
        width = block if index else block // cuts
        columns = pl.ds(pl.multiple_of(other(me, m) * block + cut * width, width), width)
        sem = g_sem.at[cuts - 1 + index if index else cut]
        return pltpu.make_async_copy(g_hbm.at[:, columns], g_ref.at[m, :, pl.ds(cut * width, width)], sem)

    def load_basis(a):
        columns = pl.ds(a * half, half)
        return pltpu.make_async_copy(b_hbm.at[:, columns], b_ref.at[:, columns], b_sem.at[a])

    def copy(src, dst, send, recv, to):
        return pltpu.make_async_remote_copy(
            src_ref=src, dst_ref=dst, send_sem=send, recv_sem=recv,
            device_id=to, device_id_type=pl.DeviceIdType.MESH,
        )

    def settle(sent, sem):
        pltpu.make_async_copy(sent, sent, sem).wait()

    def strip(h):
        return pl.ds(h * sub, sub)

    schedule = []
    for phase in range(bits):
        lanes = []
        for h in range(2):
            order = orders[h]
            masks = [m for m in range(n) if first_bit(m, order) == phase]
            masks.sort(key=lambda m: first_bit(m & ~(1 << order[phase]), order))
            lanes.append([(h, phase, m, m & ~(1 << order[phase])) for m in masks])
        schedule.append([move for pair in zip(*lanes) for move in pair])
    slot = {}
    for phase_moves in schedule:
        for h, phase, m, there in phase_moves:
            slot[h, phase, there] = len(slot)

    def stage(h, m):
        return first_bit(m, orders[h]) % bits

    stages = [stage(h, there) for h, _, there in slot]

    class Halving:
        def __init__(self, a, parts, lands, sends, recvs, early):
            self.a, self.parts, self.lands, self.sends, self.recvs = a, parts, lands, sends, recvs
            self.early = early
            self.landed = set()

        def make(self, h, phase, m, there):
            at = slot[h, phase, there]
            count = cuts if self.early and (h, phase, m, there) in schedule[0][:2] else 1
            width = block // count
            return [
                copy(
                    self.parts.at[self.a, m, strip(h), pl.ds(cut * width, width)],
                    self.lands.at[self.a, at, :, pl.ds(cut * width, width)],
                    self.sends.at[self.a], self.recvs.at[self.a, stage(h, there)], partner(orders[h][phase]),
                )
                for cut in range(count)
            ]

        def absorb(self, h, phase, m):
            group = stage(h, m)
            if group not in self.landed:
                self.landed.add(group)
                settle(land.at[0, pl.ds(0, stages.count(group))], self.recvs.at[self.a, group])
            rows = slice(h * sub, (h + 1) * sub)
            self.parts[self.a, m, rows] = self.parts[self.a, m, rows] + self.lands[self.a, slot[h, phase, m]]

        def send(self, moves):
            for move in moves:
                for item in self.make(*move):
                    item.start()

        def forward(self):
            for phase in range(1, bits):
                for move in schedule[phase]:
                    for earlier in range(phase):
                        self.absorb(move[0], earlier, move[2])
                    self.send([move])

        def finish(self):
            for phase in range(bits):
                for h in range(2):
                    self.absorb(h, phase, 0)

        def drain(self):
            settle(self.parts.at[self.a, pl.ds(0, n - 1)], self.sends.at[self.a])

    first = [Halving(a, part, land, s_rs, r_rs, a == 0) for a in range(2)]
    second = [Halving(a, part2, land2, s_rs2, r_rs2, False) for a in range(2)]

    spread = []
    for h in range(2):
        held = [0]
        for bit in reversed(orders[h]):
            for m in list(held):
                spread.append((h, bit, m))
                held.append(m | 1 << bit)
    passed = {(h, m) for h, _, m in spread}
    groups = {}
    for h, bit, m in spread:
        there = m | 1 << bit
        level = bin(there).count("1")
        groups[h, there] = 2 * level - 2 + ((h, there) not in passed)
    names = sorted(set(groups.values()))
    groups = {key: names.index(value) for key, value in groups.items()}
    own = [item for pair in zip(*[[s for s in spread if s[0] == h and s[2] == 0] for h in range(2)]) for item in pair]
    relayed = sorted((s for s in spread if s[2]), key=lambda s: bin(s[2]).count("1"))

    def spread_copy(a, h, bit, m):
        src = part.at[a, 0, strip(h)] if m == 0 else full.at[a, m, strip(h)]
        return copy(src, full.at[a, m | 1 << bit, strip(h)], s_ag.at[a], r_ag.at[a, groups[h, m | 1 << bit]], partner(bit))

    arrived = set()

    def take(a, h, m):
        if m and (a, groups[h, m]) not in arrived:
            arrived.add((a, groups[h, m]))
            count = list(groups.values()).count(groups[h, m])
            settle(land.at[0, pl.ds(0, count)], r_ag.at[a, groups[h, m]])

    def relay(a):
        for h, bit, m in relayed:
            take(a, h, m)
            spread_copy(a, h, bit, m).start()

    tile = 256 if depth % 256 == 0 else 64
    masks = sorted(range(n), key=lambda v: bin(v).count("1"))

    largest = {}

    def add_power(a, m):
        for h in range(2):
            take(a, h, m)
        held = part[a, 0] if m == 0 else full[a, m]
        inner[a, m] = held.astype(BF16)
        peak = jnp.max(jnp.abs(held), axis=0, keepdims=True)
        largest[a] = peak if m == 0 else jnp.maximum(largest[a], peak)
        if m == masks[-1]:
            scale = scale_of(jnp.max(largest[a], axis=1, keepdims=True))
        for at in range(0, depth, tile):
            rows = slice(at, at + tile)
            term = dot_t(inner[a, m], g_ref[m, rows, :])
            if m:
                term = rough[a, :, rows] + term
            if m == masks[-1]:
                power[a * half : (a + 1) * half, rows] = (term * scale).astype(BF16)
            else:
                rough[a, :, rows] = term

    grams = [(gram_a, gram_a_land), (gram_b, gram_b_land)]

    def gram_copy(a, phase, h):
        held, landed = grams[a]
        extent = held.shape[1] // 2
        rows = pl.ds(h * extent, extent)
        return copy(
            held.at[phase, rows], landed.at[phase, rows],
            s_gr.at[a], r_gr.at[a, phase], partner(orders[h][phase]),
        )

    def gram_send(a, phase):
        for h in range(2):
            gram_copy(a, phase, h).start()

    def gram_add(a, phase):
        held, landed = grams[a]
        settle(landed.at[phase], r_gr.at[a, phase])
        held[phase + 1] = held[phase] + landed[phase]

    def total_copy(at):
        return copy(total.at[at], total_land.at[at], s_tot.at[0], r_tot.at[at], rounds[at][1])

    def total_start(at):
        if at == len(rounds):
            return
        if rounds[at][0] == SWAP:
            total_copy(at).start()
        else:
            pl.when(inside)(lambda: total_copy(at).start())

    def total_next(at):
        if at >= len(rounds):
            return
        kind = rounds[at][0]

        def add():
            total_copy(at).wait()
            total[at + 1] = total[at] + total_land[at]

        def give():
            total_copy(at).wait_send()
            total[at + 1] = total[at]

        def accept():
            total_copy(at).wait_recv()
            total[at + 1] = total_land[at]

        if kind == SWAP:
            add()
        elif kind == ACROSS:
            pl.when(inside)(add)
        else:
            pl.when(inside)(give)
            pl.when(jnp.logical_not(inside))(accept)
        total_start(at + 1)

    wanted = [move[2] for move in schedule[0]] + list(range(n))
    wanted = sorted(range(n), key=wanted.index)
    load_basis(0).start()
    for cut in range(cuts):
        load(0, cut).start()
    span = 128 if depth % 128 == 0 else depth

    def turn_basis(a):
        for at in range(0, depth, span):
            bt[a * half : (a + 1) * half, at : at + span] = b_ref[at : at + span, a * half : (a + 1) * half].T

    load_basis(0).wait()
    for index in range(1, n):
        load(index).start()
    load_basis(1).start()
    turn_basis(0)

    def inner_part(a, m):
        part[a, m] = dot(bt[a * half : (a + 1) * half, :], g_ref[m])

    opening = schedule[0][:2]
    rest = schedule[0][2:]
    for cut in range(cuts):
        load(0, cut).wait()
        columns = slice(cut * (block // cuts), (cut + 1) * (block // cuts))
        part[0, wanted[0], :, columns] = dot(bt[:half, :], g_ref[wanted[0], :, columns])
        if cut == 0:
            pl.semaphore_wait(barrier, greetings)
        for move in opening:
            first[0].make(*move)[cut].start()
    for index in range(1, n):
        load(index).wait()
        m = wanted[index]
        if m == wanted[-1]:
            load_basis(1).wait()
            turn_basis(1)
            inner_part(1, wanted[0])
            first[1].send(opening)
        inner_part(0, m)
        first[0].send([move for move in rest if move[2] == m])
    for m in wanted[1:]:
        inner_part(1, m)
    live = loads[0] >= 1
    refresh = jnp.logical_and(live, flags[0] == 1)
    first[0].forward()
    first[1].send(rest)

    def squares_of(step, sums):
        rows = pl.ds(pl.multiple_of(step * 16, 16), 16)
        for m in range(n):
            piece = g_ref[m, rows, :].astype(F32)
            sums = sums + piece * piece
        return sums

    sums = lax.fori_loop(0, depth // 16, squares_of, jnp.zeros((16, block), F32))
    total_sq = jnp.where(live, jnp.sum(sums), 0.0)
    count = jnp.where(jnp.logical_and(live, me == 0), 1.0, 0.0)
    lane = lax.broadcasted_iota(jnp.int32, (1, 128), 1)
    total[0] = jnp.where(lane == 0, total_sq, jnp.where(lane == 1, count, 0.0))
    total_start(0)
    first[1].forward()
    total_next(0)
    first[0].finish()
    for item in own:
        spread_copy(0, *item).start()
    add_power(0, 0)
    total_next(1)
    first[1].finish()
    for item in own[:2]:
        spread_copy(1, *item).start()
    total_next(2)
    add_power(1, 0)
    relay(0)
    for item in own[2:]:
        spread_copy(1, *item).start()
    relay(1)
    total_next(3)
    for m in masks[1:]:
        add_power(0, m)
    gram_a[0] = pack(dot_t(power[0:half, :], power[0:half, :]))
    gram_send(0, 0)

    def cross_part(a):
        for m in wanted:
            part2[a, m] = dot(power[a * half : (a + 1) * half, :], g_ref[m])

    cross_part(0)
    second[0].send(opening)
    for m in masks[1:-1]:
        add_power(1, m)
    for phase in range(bits - 1):
        gram_add(0, phase)
        gram_send(0, phase + 1)
    add_power(1, masks[-1])
    total_next(4)
    both = dot_t(power[...], power[half:size, :])
    gram_b[0] = jnp.concatenate([both[:half], pack(both[half:])], axis=0)
    gram_send(1, 0)
    second[0].send(rest)
    cross_part(1)
    gram_add(0, bits - 1)
    panels = half // PANEL
    work[...] = unpack(gram_a[bits])
    panel_steps(work, 0, panels // 4)
    for phase in range(bits - 1):
        gram_add(1, phase)
        gram_send(1, phase + 1)
    second[1].send(opening)
    second[0].forward()
    second[1].send(rest)
    panel_steps(work, panels // 4, panels)

    def write_fresh(a, pieces):
        for at in range(0, depth, tile):
            rows = slice(at, at + tile)
            columns = slice(a * half, (a + 1) * half)
            left = power[0 : (a + 1) * half, rows].T
            value = dot(left, pieces[2]) + dot(left, pieces[1]) + dot(left, pieces[0])
            kept = jnp.where(live, b_ref[rows, columns].astype(F32), 0.0)
            fresh[rows, columns] = jnp.where(refresh, value, kept)

    inverse_a = lower_of(work)
    write_fresh(0, pieces_of(inverse_a.T, 3))
    gram_add(1, bits - 1)
    upper = dot(inverse_a, gram_b[bits, :half], HIGHEST)
    work[...] = unpack(gram_b[bits, half:]) - dot(upper.T, upper, HIGHEST)
    panel_steps(work, 0, panels * 5 // 8)
    second[1].forward()
    panel_steps(work, panels * 5 // 8, panels)
    second[0].finish()
    turned_a = dot(inverse_a, part2[0, 0], HIGHEST)
    inverse_b = lower_of(work)
    mixed = -dot(inverse_b, dot(upper.T, inverse_a, HIGHEST), HIGHEST)
    write_fresh(1, pieces_of(jnp.concatenate([mixed, inverse_b], axis=1).T, 3))
    for at in range(5, len(rounds)):
        total_next(at)
    final = total[len(rounds)]
    norm = lax.rsqrt(final[0:1, 0:1] / (final[0:1, 1:2] * entries) + 1e-6)

    def write_rot(a, turned):
        rot[a * half : (a + 1) * half, :] = jnp.where(refresh, turned, jnp.where(live, part[a, 0], 0.0)) * norm

    write_rot(0, turned_a)
    write_rot(1, dot(mixed, part2[0, 0], HIGHEST))
    pair[...] = jnp.concatenate(pieces_of(jnp.where(refresh, inverse_b * norm, 0.0), 2), axis=1)
    second[1].finish()
    cross[...] = jnp.where(refresh, part2[1, 0], 0.0)
    for a in range(2):
        first[a].drain()
        second[a].drain()
        settle(full.at[a, pl.ds(0, n - 1)], s_ag.at[a])
        settle(grams[a][0].at[pl.ds(0, bits)], s_gr.at[a])


def write_out(fresh, rot, pair, cross, fresh_hbm, rot_hbm, last, fresh_sem, rot_sem):
    extent = fresh.shape[0] // PARTS
    half = cross.shape[0]
    copies = [pltpu.make_async_copy(rot.at[pl.ds(0, half)], rot_hbm.at[0, pl.ds(0, half)], rot_sem.at[0])]
    for at in range(PARTS):
        rows = pl.ds(at * extent, extent)
        copies.append(pltpu.make_async_copy(fresh.at[rows], fresh_hbm.at[0, rows], fresh_sem.at[at]))
    for item in copies:
        item.start()
    top, low = pieces_of(cross[...], 2)
    turned = dot(pair[...], jnp.concatenate([low, low], axis=0)) + dot(pair[...], jnp.concatenate([top, top], axis=0))
    last[...] = rot[half:, :] + turned
    copies.append(pltpu.make_async_copy(last, rot_hbm.at[0, pl.ds(half, half)], rot_sem.at[1]))
    copies[-1].start()
    for item in copies:
        item.wait()


def on_device(n, experts, grads, basis, loads, flags):
    _, depth, wide = grads.shape
    size = basis.shape[2]
    half = size // 2
    block = wide // n
    bits = n.bit_length() - 1
    rounds = bits + experts.bit_length() - 1 + (experts == 8)
    moves = 2 * (n - 1)
    packed = half * 5 // 8
    cuts = 2 if block % 256 == 0 else 1
    anywhere = pl.BlockSpec(memory_space=pl.ANY)
    vmem = pl.BlockSpec(memory_space=pltpu.VMEM)
    chunk = (half // 2, block)
    dma = pltpu.SemaphoreType.DMA
    results = pl.pallas_call(
        functools.partial(kernel, n, experts, float(depth * n * wide)),
        out_shape=(
            pltpu.VMEM((depth, size), F32), pltpu.VMEM((size, block), F32),
            pltpu.VMEM((half, size), BF16), pltpu.VMEM((half, block), F32),
        ),
        in_specs=[pl.BlockSpec(memory_space=pltpu.HBM)] * 2 + [pl.BlockSpec(memory_space=pltpu.SMEM)] * 2,
        out_specs=(vmem, vmem, vmem, vmem),
        scratch_shapes=[
            pltpu.VMEM((n, depth, block), BF16),
            pltpu.VMEM((depth, size), BF16),
            pltpu.VMEM((size, depth), BF16),
            pltpu.VMEM((2, n, half, block), F32),
            pltpu.VMEM((2, moves, *chunk), F32),
            pltpu.VMEM((2, n, half, block), F32),
            pltpu.VMEM((2, n, half, block), BF16),
            pltpu.VMEM((2, half, depth), F32),
            pltpu.VMEM((size, depth), BF16),
            pltpu.VMEM((2, n, half, block), F32),
            pltpu.VMEM((2, moves, *chunk), F32),
            pltpu.VMEM((bits + 1, packed, half), F32),
            pltpu.VMEM((bits, packed, half), F32),
            pltpu.VMEM((bits + 1, half + packed, half), F32),
            pltpu.VMEM((bits, half + packed, half), F32),
            pltpu.VMEM((half, half), F32),
            pltpu.VMEM((rounds + 1, 1, 128), F32),
            pltpu.VMEM((rounds, 1, 128), F32),
            dma((n - 1 + cuts,)), dma((2,)),
            dma((2,)), dma((2, bits)), dma((2,)), dma((2, 2 * bits - 1)), dma((2,)), dma((2, bits)),
            dma((2,)), dma((2, bits)), dma((1,)), dma((rounds,)),
        ],
        compiler_params=pltpu.CompilerParams(
            collective_id=0, has_side_effects=True, vmem_limit_bytes=32 * 1024 * 1024
        ),
    )(*[pltpu.with_memory_space_constraint(x, pltpu.HBM) for x in (grads[0], basis[0])], loads, flags)
    return pl.pallas_call(
        write_out,
        out_shape=(
            jax.ShapeDtypeStruct((1, depth, size), F32),
            jax.ShapeDtypeStruct((1, size, block), F32),
        ),
        in_specs=[vmem] * 4,
        out_specs=(anywhere, anywhere),
        scratch_shapes=[pltpu.VMEM((half, block), F32), dma((PARTS,)), dma((2,))],
        compiler_params=pltpu.CompilerParams(vmem_limit_bytes=16 * 1024 * 1024),
    )(*results)


def solution(mesh):
    placed = (P("expert", "row", None), P("expert", "row", None), P("expert"), P("expert"))
    return jax.shard_map(
        functools.partial(on_device, mesh.shape["row"], mesh.shape["expert"]),
        mesh=mesh,
        in_specs=placed,
        out_specs=(P("expert", "row", None), P("expert", None, "row")),
        check_vma=False,
    )
```

```python
import functools

import jax
import jax.numpy as jnp
from jax import lax
from jax.experimental import pallas as pl
from jax.experimental.pallas import tpu as pltpu
from jax.sharding import PartitionSpec as P

PANEL = 16
PARTS = 4
SWAP, ACROSS, OUTWARD = range(3)
HIGHEST = lax.Precision.HIGHEST
F32 = jnp.float32
BF16 = jnp.bfloat16


def dot(a, b, precision=None):
    return lax.dot_general(a, b, (((1,), (0,)), ((), ())), precision=precision, preferred_element_type=F32)


def dot_t(a, b, precision=None):
    return lax.dot_general(a, b, (((1,), (1,)), ((), ())), precision=precision, preferred_element_type=F32)


def pieces_of(x, count):
    pieces = []
    for _ in range(count):
        pieces.append(x.astype(BF16))
        x = x - pieces[-1].astype(F32)
    return pieces


def scale_of(peak):
    scale = jnp.where(peak > 2.0**10, 2.0**-40, jnp.where(peak < 2.0**-10, 2.0**40, 1.0))
    return jnp.where(peak > 2.0**35, 2.0**-80, jnp.where(peak < 2.0**-35, 2.0**80, scale))


def first_bit(mask, order):
    for phase, bit in enumerate(order):
        if mask >> bit & 1:
            return phase
    return len(order)


def panel_step(work, step):
    size = work.shape[0]
    panel = work[0:PANEL, :]
    rows = lax.broadcasted_iota(jnp.int32, (PANEL, 128), 0)
    lanes = lax.broadcasted_iota(jnp.int32, (PANEL, 128), 1)
    columns = [jnp.broadcast_to(panel[:, j : j + 1], (PANEL, 128)) for j in range(PANEL)]
    pieces = [panel[:, at : at + 128] for at in range(0, size, 128)]
    unit = (rows == lanes).astype(F32)
    root = jnp.zeros((PANEL, 128), F32)
    for j in range(PANEL):
        inverse_root = lax.rsqrt(columns[j][j : j + 1, :])
        root = jnp.where(rows == j, inverse_root, root)
        factor = jnp.where(rows > j, columns[j] * (inverse_root * inverse_root), 0.0)
        for k in range(j + 1, PANEL):
            columns[k] = columns[k] - factor * columns[k][j : j + 1, :]
        pieces = [piece - factor * piece[j : j + 1, :] for piece in pieces]
        unit = unit - factor * unit[j : j + 1, :]
    scaled = [root * piece for piece in pieces]
    full = jnp.concatenate([jnp.where(lanes < PANEL, root * unit, scaled[0])] + scaled[1:], axis=1)
    where = lax.broadcasted_iota(jnp.int32, (PANEL, size), 1)
    open_columns = jnp.logical_and(where >= PANEL, where < size - PANEL * step)
    left = jnp.where(open_columns, jnp.concatenate(scaled, axis=1), 0.0)
    update = dot(left.T, full, HIGHEST)
    body = work[PANEL:, :]
    ahead = lax.broadcasted_iota(jnp.int32, body.shape, 1) < PANEL
    rest = jnp.where(ahead, 0.0, body) - update[PANEL:, :]
    work[0 : size - PANEL, :] = pltpu.roll(rest, size - PANEL, 1)
    work[size - PANEL :, :] = pltpu.roll(full, size - PANEL, 1)


def pack(square):
    size = square.shape[0]
    q = size // 4
    lane = lax.broadcasted_iota(jnp.int32, (q, size), 1)
    second = jnp.where(lane < q, pltpu.roll(square[3 * q :], q, 1), square[q : 2 * q])
    third = square[2 * q : 3 * q]
    lane = lane[: q // 2]
    third = jnp.where(lane < 2 * q, pltpu.roll(third[q // 2 :], 2 * q, 1), third[: q // 2])
    return jnp.concatenate([square[:q], second, third], axis=0)


def unpack(packed):
    size = packed.shape[1]
    q = size // 4
    second, third = packed[q : 2 * q], packed[2 * q :]
    rows = [packed[:q], second, third, pltpu.roll(third, 2 * q, 1), pltpu.roll(second, size - q, 1)]
    return jnp.concatenate(rows, axis=0)


def panel_steps(work, begin, end):
    def body(step, carry):
        panel_step(work, step)
        return carry

    lax.fori_loop(begin, end, body, 0)


def lower_of(work):
    shape = work.shape
    below = lax.broadcasted_iota(jnp.int32, shape, 1) <= lax.broadcasted_iota(jnp.int32, shape, 0)
    return jnp.where(below, work[...], 0.0)


def kernel(
    n, experts, entries, g_hbm, b_hbm, loads, flags, fresh, rot, pair, cross,
    g_ref, b_ref, bt, part, land, full, inner, rough, power, part2, land2,
    gram_a, gram_a_land, gram_b, gram_b_land, work, total, total_land,
    g_sem, b_sem,
    s_rs, r_rs, s_ag, r_ag, s_rs2, r_rs2, s_gr, r_gr, s_tot, r_tot,
):
    _, depth, block = g_ref.shape
    bits = n.bit_length() - 1
    expert_bits = experts.bit_length() - 1
    size = b_ref.shape[1]
    half = size // 2
    sub = half // 2
    me = lax.axis_index("row")
    my_expert = lax.axis_index("expert")
    orders = [tuple(range(bits)), tuple(reversed(range(bits)))]
    cuts = g_sem.shape[0] - n + 1

    def other(index, mask):
        at = index
        for bit in range(max(bits, expert_bits)):
            if mask >> bit & 1:
                at = at + (1 - 2 * (lax.rem(index // (1 << bit), 2))) * (1 << bit)
        return at

    def partner(bit):
        return {"row": other(me, 1 << bit), "expert": my_expert}

    def expert_partner(bit):
        return {"row": me, "expert": other(my_expert, 1 << bit)}

    place = my_expert // 2
    inside = jnp.logical_or(place == 1, place == 2)
    across = {"row": me, "expert": my_expert + jnp.where(place == 1, 2, -2)}
    if expert_bits == 3:
        rounds = [(SWAP, expert_partner(0)), (SWAP, expert_partner(1)), (ACROSS, across), (OUTWARD, expert_partner(1))]
    else:
        rounds = [(SWAP, expert_partner(b)) for b in range(expert_bits)]
    rounds = rounds + [(SWAP, partner(b)) for b in range(bits)]
    barrier = pltpu.get_barrier_semaphore()

    def greet(peer):
        pl.semaphore_signal(barrier, inc=1, device_id=peer, device_id_type=pl.DeviceIdType.MESH)

    greetings = 0
    for kind, peer in rounds:
        if kind == SWAP:
            greet(peer)
            greetings += 1
    if expert_bits == 3:
        pl.when(inside)(lambda: greet(across))
        greetings = greetings + inside.astype(jnp.int32)

    def load(index, cut=0):
        m = wanted[index]
        width = block if index else block // cuts
        columns = pl.ds(pl.multiple_of(other(me, m) * block + cut * width, width), width)
        sem = g_sem.at[cuts - 1 + index if index else cut]
        return pltpu.make_async_copy(g_hbm.at[:, columns], g_ref.at[m, :, pl.ds(cut * width, width)], sem)

    def load_basis(a):
        columns = pl.ds(a * half, half)
        return pltpu.make_async_copy(b_hbm.at[:, columns], b_ref.at[:, columns], b_sem.at[a])

    def copy(src, dst, send, recv, to):
        return pltpu.make_async_remote_copy(
            src_ref=src, dst_ref=dst, send_sem=send, recv_sem=recv,
            device_id=to, device_id_type=pl.DeviceIdType.MESH,
        )

    def settle(sent, sem):
        pltpu.make_async_copy(sent, sent, sem).wait()

    def strip(h):
        return pl.ds(h * sub, sub)

    schedule = []
    for phase in range(bits):
        lanes = []
        for h in range(2):
            order = orders[h]
            masks = [m for m in range(n) if first_bit(m, order) == phase]
            masks.sort(key=lambda m: first_bit(m & ~(1 << order[phase]), order))
            lanes.append([(h, phase, m, m & ~(1 << order[phase])) for m in masks])
        schedule.append([move for pair in zip(*lanes) for move in pair])
    slot = {}
    for phase_moves in schedule:
        for h, phase, m, there in phase_moves:
            slot[h, phase, there] = len(slot)

    def stage(h, m):
        return first_bit(m, orders[h]) % bits

    stages = [stage(h, there) for h, _, there in slot]

    class Halving:
        def __init__(self, a, parts, lands, sends, recvs, early):
            self.a, self.parts, self.lands, self.sends, self.recvs = a, parts, lands, sends, recvs
            self.early = early
            self.landed = set()

        def make(self, h, phase, m, there):
            at = slot[h, phase, there]
            count = cuts if self.early and (h, phase, m, there) in schedule[0][:2] else 1
            width = block // count
            return [
                copy(
                    self.parts.at[self.a, m, strip(h), pl.ds(cut * width, width)],
                    self.lands.at[self.a, at, :, pl.ds(cut * width, width)],
                    self.sends.at[self.a], self.recvs.at[self.a, stage(h, there)], partner(orders[h][phase]),
                )
                for cut in range(count)
            ]

        def absorb(self, h, phase, m):
            group = stage(h, m)
            if group not in self.landed:
                self.landed.add(group)
                settle(land.at[0, pl.ds(0, stages.count(group))], self.recvs.at[self.a, group])
            rows = slice(h * sub, (h + 1) * sub)
            self.parts[self.a, m, rows] = self.parts[self.a, m, rows] + self.lands[self.a, slot[h, phase, m]]

        def send(self, moves):
            for move in moves:
                for item in self.make(*move):
                    item.start()

        def forward(self):
            for phase in range(1, bits):
                for move in schedule[phase]:
                    for earlier in range(phase):
                        self.absorb(move[0], earlier, move[2])
                    self.send([move])

        def finish(self):
            for phase in range(bits):
                for h in range(2):
                    self.absorb(h, phase, 0)

        def drain(self):
            settle(self.parts.at[self.a, pl.ds(0, n - 1)], self.sends.at[self.a])

    first = [Halving(a, part, land, s_rs, r_rs, a == 0) for a in range(2)]
    second = [Halving(a, part2, land2, s_rs2, r_rs2, False) for a in range(2)]

    spread = []
    for h in range(2):
        held = [0]
        for bit in reversed(orders[h]):
            for m in list(held):
                spread.append((h, bit, m))
                held.append(m | 1 << bit)
    passed = {(h, m) for h, _, m in spread}
    groups = {}
    for h, bit, m in spread:
        there = m | 1 << bit
        level = bin(there).count("1")
        groups[h, there] = 2 * level - 2 + ((h, there) not in passed)
    names = sorted(set(groups.values()))
    groups = {key: names.index(value) for key, value in groups.items()}
    own = [item for pair in zip(*[[s for s in spread if s[0] == h and s[2] == 0] for h in range(2)]) for item in pair]
    relayed = sorted((s for s in spread if s[2]), key=lambda s: bin(s[2]).count("1"))

    def spread_copy(a, h, bit, m):
        src = part.at[a, 0, strip(h)] if m == 0 else full.at[a, m, strip(h)]
        return copy(src, full.at[a, m | 1 << bit, strip(h)], s_ag.at[a], r_ag.at[a, groups[h, m | 1 << bit]], partner(bit))

    arrived = set()

    def take(a, h, m):
        if m and (a, groups[h, m]) not in arrived:
            arrived.add((a, groups[h, m]))
            count = list(groups.values()).count(groups[h, m])
            settle(land.at[0, pl.ds(0, count)], r_ag.at[a, groups[h, m]])

    def relay(a):
        for h, bit, m in relayed:
            take(a, h, m)
            spread_copy(a, h, bit, m).start()

    tile = 256 if depth % 256 == 0 else 64
    masks = sorted(range(n), key=lambda v: bin(v).count("1"))

    largest = {}

    def add_power(a, m):
        for h in range(2):
            take(a, h, m)
        held = part[a, 0] if m == 0 else full[a, m]
        inner[a, m] = held.astype(BF16)
        peak = jnp.max(jnp.abs(held), axis=0, keepdims=True)
        largest[a] = peak if m == 0 else jnp.maximum(largest[a], peak)
        if m == masks[-1]:
            scale = scale_of(jnp.max(largest[a], axis=1, keepdims=True))
        for at in range(0, depth, tile):
            rows = slice(at, at + tile)
            term = dot_t(inner[a, m], g_ref[m, rows, :])
            if m:
                term = rough[a, :, rows] + term
            if m == masks[-1]:
                power[a * half : (a + 1) * half, rows] = (term * scale).astype(BF16)
            else:
                rough[a, :, rows] = term

    grams = [(gram_a, gram_a_land), (gram_b, gram_b_land)]

    def gram_copy(a, phase, h):
        held, landed = grams[a]
        extent = held.shape[1] // 2
        rows = pl.ds(h * extent, extent)
        return copy(
            held.at[phase, rows], landed.at[phase, rows],
            s_gr.at[a], r_gr.at[a, phase], partner(orders[h][phase]),
        )

    def gram_send(a, phase):
        for h in range(2):
            gram_copy(a, phase, h).start()

    def gram_add(a, phase):
        held, landed = grams[a]
        settle(landed.at[phase], r_gr.at[a, phase])
        held[phase + 1] = held[phase] + landed[phase]

    def total_copy(at):
        return copy(total.at[at], total_land.at[at], s_tot.at[0], r_tot.at[at], rounds[at][1])

    def total_start(at):
        if at == len(rounds):
            return
        if rounds[at][0] == SWAP:
            total_copy(at).start()
        else:
            pl.when(inside)(lambda: total_copy(at).start())

    def total_next(at):
        if at >= len(rounds):
            return
        kind = rounds[at][0]

        def add():
            total_copy(at).wait()
            total[at + 1] = total[at] + total_land[at]

        def give():
            total_copy(at).wait_send()
            total[at + 1] = total[at]

        def accept():
            total_copy(at).wait_recv()
            total[at + 1] = total_land[at]

        if kind == SWAP:
            add()
        elif kind == ACROSS:
            pl.when(inside)(add)
        else:
            pl.when(inside)(give)
            pl.when(jnp.logical_not(inside))(accept)
        total_start(at + 1)

    wanted = [move[2] for move in schedule[0]] + list(range(n))
    wanted = sorted(range(n), key=wanted.index)
    load_basis(0).start()
    for cut in range(cuts):
        load(0, cut).start()
    span = 128 if depth % 128 == 0 else depth

    def turn_basis(a):
        for at in range(0, depth, span):
            bt[a * half : (a + 1) * half, at : at + span] = b_ref[at : at + span, a * half : (a + 1) * half].T

    load_basis(0).wait()
    for index in range(1, n):
        load(index).start()
    load_basis(1).start()
    turn_basis(0)

    def inner_part(a, m):
        part[a, m] = dot(bt[a * half : (a + 1) * half, :], g_ref[m])

    opening = schedule[0][:2]
    rest = schedule[0][2:]
    for cut in range(cuts):
        load(0, cut).wait()
        columns = slice(cut * (block // cuts), (cut + 1) * (block // cuts))
        part[0, wanted[0], :, columns] = dot(bt[:half, :], g_ref[wanted[0], :, columns])
        if cut == 0:
            pl.semaphore_wait(barrier, greetings)
        for move in opening:
            first[0].make(*move)[cut].start()
    for index in range(1, n):
        load(index).wait()
        m = wanted[index]
        if m == wanted[-1]:
            load_basis(1).wait()
            turn_basis(1)
            inner_part(1, wanted[0])
            first[1].send(opening)
        inner_part(0, m)
        first[0].send([move for move in rest if move[2] == m])
    for m in wanted[1:]:
        inner_part(1, m)
    live = loads[0] >= 1
    refresh = jnp.logical_and(live, flags[0] == 1)
    first[0].forward()
    first[1].send(rest)

    def squares_of(step, sums):
        rows = pl.ds(pl.multiple_of(step * 16, 16), 16)
        for m in range(n):
            piece = g_ref[m, rows, :].astype(F32)
            sums = sums + piece * piece
        return sums

    sums = lax.fori_loop(0, depth // 16, squares_of, jnp.zeros((16, block), F32))
    total_sq = jnp.where(live, jnp.sum(sums), 0.0)
    count = jnp.where(jnp.logical_and(live, me == 0), 1.0, 0.0)
    lane = lax.broadcasted_iota(jnp.int32, (1, 128), 1)
    total[0] = jnp.where(lane == 0, total_sq, jnp.where(lane == 1, count, 0.0))
    total_start(0)
    first[1].forward()
    total_next(0)
    first[0].finish()
    for item in own:
        spread_copy(0, *item).start()
    add_power(0, 0)
    total_next(1)
    first[1].finish()
    for item in own[:2]:
        spread_copy(1, *item).start()
    total_next(2)
    add_power(1, 0)
    relay(0)
    for item in own[2:]:
        spread_copy(1, *item).start()
    relay(1)
    total_next(3)
    for m in masks[1:]:
        add_power(0, m)
    gram_a[0] = pack(dot_t(power[0:half, :], power[0:half, :]))
    gram_send(0, 0)

    def cross_part(a):
        for m in wanted:
            part2[a, m] = dot(power[a * half : (a + 1) * half, :], g_ref[m])

    cross_part(0)
    second[0].send(opening)
    for m in masks[1:-1]:
        add_power(1, m)
    for phase in range(bits - 1):
        gram_add(0, phase)
        gram_send(0, phase + 1)
    add_power(1, masks[-1])
    total_next(4)
    both = dot_t(power[...], power[half:size, :])
    gram_b[0] = jnp.concatenate([both[:half], pack(both[half:])], axis=0)
    gram_send(1, 0)
    second[0].send(rest)
    cross_part(1)
    gram_add(0, bits - 1)
    panels = half // PANEL
    work[...] = unpack(gram_a[bits])
    panel_steps(work, 0, panels // 4)
    for phase in range(bits - 1):
        gram_add(1, phase)
        gram_send(1, phase + 1)
    second[1].send(opening)
    second[0].forward()
    second[1].send(rest)
    panel_steps(work, panels // 4, panels)

    def write_fresh(a, pieces):
        for at in range(0, depth, tile):
            rows = slice(at, at + tile)
            columns = slice(a * half, (a + 1) * half)
            left = power[0 : (a + 1) * half, rows].T
            value = dot(left, pieces[2]) + dot(left, pieces[1]) + dot(left, pieces[0])
            kept = jnp.where(live, b_ref[rows, columns].astype(F32), 0.0)
            fresh[rows, columns] = jnp.where(refresh, value, kept)

    inverse_a = lower_of(work)
    write_fresh(0, pieces_of(inverse_a.T, 3))
    gram_add(1, bits - 1)
    upper = dot(inverse_a, gram_b[bits, :half], HIGHEST)
    work[...] = unpack(gram_b[bits, half:]) - dot(upper.T, upper, HIGHEST)
    panel_steps(work, 0, panels * 5 // 8)
    second[1].forward()
    panel_steps(work, panels * 5 // 8, panels)
    second[0].finish()
    turned_a = dot(inverse_a, part2[0, 0], HIGHEST)
    inverse_b = lower_of(work)
    mixed = -dot(inverse_b, dot(upper.T, inverse_a, HIGHEST), HIGHEST)
    write_fresh(1, pieces_of(jnp.concatenate([mixed, inverse_b], axis=1).T, 3))
    for at in range(5, len(rounds)):
        total_next(at)
    final = total[len(rounds)]
    norm = lax.rsqrt(final[0:1, 0:1] / (final[0:1, 1:2] * entries) + 1e-6)

    def write_rot(a, turned):
        rot[a * half : (a + 1) * half, :] = jnp.where(refresh, turned, jnp.where(live, part[a, 0], 0.0)) * norm

    write_rot(0, turned_a)
    write_rot(1, dot(mixed, part2[0, 0], HIGHEST))
    pair[...] = jnp.concatenate(pieces_of(jnp.where(refresh, inverse_b * norm, 0.0), 2), axis=1)
    settle(land.at[0, pl.ds(0, stages.count(0))], r_rs2.at[1, 0])
    for h in range(2):
        rows = slice(h * sub, (h + 1) * sub)
        value = part2[1, 0, rows]
        for phase in range(bits):
            value = value + land2[1, slot[h, phase, 0]]
        cross[rows, :] = jnp.where(refresh, value, 0.0)
    for a in range(2):
        first[a].drain()
        second[a].drain()
        settle(full.at[a, pl.ds(0, n - 1)], s_ag.at[a])
        settle(grams[a][0].at[pl.ds(0, bits)], s_gr.at[a])


def write_out(fresh, rot, pair, cross, fresh_hbm, rot_hbm, last, fresh_sem, rot_sem):
    extent = fresh.shape[0] // PARTS
    half = cross.shape[0]
    copies = [pltpu.make_async_copy(rot.at[pl.ds(0, half)], rot_hbm.at[0, pl.ds(0, half)], rot_sem.at[0])]
    for at in range(PARTS):
        rows = pl.ds(at * extent, extent)
        copies.append(pltpu.make_async_copy(fresh.at[rows], fresh_hbm.at[0, rows], fresh_sem.at[at]))
    for item in copies:
        item.start()
    top, low = pieces_of(cross[...], 2)
    turned = dot(pair[...], jnp.concatenate([low, low], axis=0)) + dot(pair[...], jnp.concatenate([top, top], axis=0))
    last[...] = rot[half:, :] + turned
    copies.append(pltpu.make_async_copy(last, rot_hbm.at[0, pl.ds(half, half)], rot_sem.at[1]))
    copies[-1].start()
    for item in copies:
        item.wait()


def on_device(n, experts, grads, basis, loads, flags):
    _, depth, wide = grads.shape
    size = basis.shape[2]
    half = size // 2
    block = wide // n
    bits = n.bit_length() - 1
    rounds = bits + experts.bit_length() - 1 + (experts == 8)
    moves = 2 * (n - 1)
    packed = half * 5 // 8
    cuts = 2 if block % 256 == 0 else 1
    anywhere = pl.BlockSpec(memory_space=pl.ANY)
    vmem = pl.BlockSpec(memory_space=pltpu.VMEM)
    chunk = (half // 2, block)
    dma = pltpu.SemaphoreType.DMA
    results = pl.pallas_call(
        functools.partial(kernel, n, experts, float(depth * n * wide)),
        out_shape=(
            pltpu.VMEM((depth, size), F32), pltpu.VMEM((size, block), F32),
            pltpu.VMEM((half, size), BF16), pltpu.VMEM((half, block), F32),
        ),
        in_specs=[pl.BlockSpec(memory_space=pltpu.HBM)] * 2 + [pl.BlockSpec(memory_space=pltpu.SMEM)] * 2,
        out_specs=(vmem, vmem, vmem, vmem),
        scratch_shapes=[
            pltpu.VMEM((n, depth, block), BF16),
            pltpu.VMEM((depth, size), BF16),
            pltpu.VMEM((size, depth), BF16),
            pltpu.VMEM((2, n, half, block), F32),
            pltpu.VMEM((2, moves, *chunk), F32),
            pltpu.VMEM((2, n, half, block), F32),
            pltpu.VMEM((2, n, half, block), BF16),
            pltpu.VMEM((2, half, depth), F32),
            pltpu.VMEM((size, depth), BF16),
            pltpu.VMEM((2, n, half, block), F32),
            pltpu.VMEM((2, moves, *chunk), F32),
            pltpu.VMEM((bits + 1, packed, half), F32),
            pltpu.VMEM((bits, packed, half), F32),
            pltpu.VMEM((bits + 1, half + packed, half), F32),
            pltpu.VMEM((bits, half + packed, half), F32),
            pltpu.VMEM((half, half), F32),
            pltpu.VMEM((rounds + 1, 1, 128), F32),
            pltpu.VMEM((rounds, 1, 128), F32),
            dma((n - 1 + cuts,)), dma((2,)),
            dma((2,)), dma((2, bits)), dma((2,)), dma((2, 2 * bits - 1)), dma((2,)), dma((2, bits)),
            dma((2,)), dma((2, bits)), dma((1,)), dma((rounds,)),
        ],
        compiler_params=pltpu.CompilerParams(
            collective_id=0, has_side_effects=True, vmem_limit_bytes=32 * 1024 * 1024
        ),
    )(*[pltpu.with_memory_space_constraint(x, pltpu.HBM) for x in (grads[0], basis[0])], loads, flags)
    return pl.pallas_call(
        write_out,
        out_shape=(
            jax.ShapeDtypeStruct((1, depth, size), F32),
            jax.ShapeDtypeStruct((1, size, block), F32),
        ),
        in_specs=[vmem] * 4,
        out_specs=(anywhere, anywhere),
        scratch_shapes=[pltpu.VMEM((half, block), F32), dma((PARTS,)), dma((2,))],
        compiler_params=pltpu.CompilerParams(vmem_limit_bytes=16 * 1024 * 1024),
    )(*results)


def solution(mesh):
    placed = (P("expert", "row", None), P("expert", "row", None), P("expert"), P("expert"))
    return jax.shard_map(
        functools.partial(on_device, mesh.shape["row"], mesh.shape["expert"]),
        mesh=mesh,
        in_specs=placed,
        out_specs=(P("expert", "row", None), P("expert", None, "row")),
        check_vma=False,
    )
```

```python
import functools

import jax
import jax.numpy as jnp
from jax import lax
from jax.experimental import pallas as pl
from jax.experimental.pallas import tpu as pltpu
from jax.sharding import PartitionSpec as P

PANEL = 16
PARTS = 4
SWAP, ACROSS, OUTWARD = range(3)
HIGHEST = lax.Precision.HIGHEST
F32 = jnp.float32
BF16 = jnp.bfloat16


def dot(a, b, precision=None):
    return lax.dot_general(a, b, (((1,), (0,)), ((), ())), precision=precision, preferred_element_type=F32)


def dot_t(a, b, precision=None):
    return lax.dot_general(a, b, (((1,), (1,)), ((), ())), precision=precision, preferred_element_type=F32)


def pieces_of(x, count):
    pieces = []
    for _ in range(count):
        pieces.append(x.astype(BF16))
        x = x - pieces[-1].astype(F32)
    return pieces


def scale_of(peak):
    scale = jnp.where(peak > 2.0**10, 2.0**-40, jnp.where(peak < 2.0**-10, 2.0**40, 1.0))
    return jnp.where(peak > 2.0**35, 2.0**-80, jnp.where(peak < 2.0**-35, 2.0**80, scale))


def first_bit(mask, order):
    for phase, bit in enumerate(order):
        if mask >> bit & 1:
            return phase
    return len(order)


def panel_step(work, step):
    size = work.shape[0]
    panel = work[0:PANEL, :]
    rows = lax.broadcasted_iota(jnp.int32, (PANEL, 128), 0)
    lanes = lax.broadcasted_iota(jnp.int32, (PANEL, 128), 1)
    columns = [jnp.broadcast_to(panel[:, j : j + 1], (PANEL, 128)) for j in range(PANEL)]
    pieces = [panel[:, at : at + 128] for at in range(0, size, 128)]
    unit = (rows == lanes).astype(F32)
    root = jnp.zeros((PANEL, 128), F32)
    for j in range(PANEL):
        inverse_root = lax.rsqrt(columns[j][j : j + 1, :])
        root = jnp.where(rows == j, inverse_root, root)
        factor = jnp.where(rows > j, columns[j] * (inverse_root * inverse_root), 0.0)
        for k in range(j + 1, PANEL):
            columns[k] = columns[k] - factor * columns[k][j : j + 1, :]
        pieces = [piece - factor * piece[j : j + 1, :] for piece in pieces]
        unit = unit - factor * unit[j : j + 1, :]
    scaled = [root * piece for piece in pieces]
    full = jnp.concatenate([jnp.where(lanes < PANEL, root * unit, scaled[0])] + scaled[1:], axis=1)
    where = lax.broadcasted_iota(jnp.int32, (PANEL, size), 1)
    open_columns = jnp.logical_and(where >= PANEL, where < size - PANEL * step)
    left = jnp.where(open_columns, jnp.concatenate(scaled, axis=1), 0.0)
    update = dot(left.T, full, HIGHEST)
    body = work[PANEL:, :]
    ahead = lax.broadcasted_iota(jnp.int32, body.shape, 1) < PANEL
    rest = jnp.where(ahead, 0.0, body) - update[PANEL:, :]
    work[0 : size - PANEL, :] = pltpu.roll(rest, size - PANEL, 1)
    work[size - PANEL :, :] = pltpu.roll(full, size - PANEL, 1)


def pack(square):
    size = square.shape[0]
    q = size // 4
    lane = lax.broadcasted_iota(jnp.int32, (q, size), 1)
    second = jnp.where(lane < q, pltpu.roll(square[3 * q :], q, 1), square[q : 2 * q])
    third = square[2 * q : 3 * q]
    lane = lane[: q // 2]
    third = jnp.where(lane < 2 * q, pltpu.roll(third[q // 2 :], 2 * q, 1), third[: q // 2])
    return jnp.concatenate([square[:q], second, third], axis=0)


def unpack(packed):
    size = packed.shape[1]
    q = size // 4
    second, third = packed[q : 2 * q], packed[2 * q :]
    rows = [packed[:q], second, third, pltpu.roll(third, 2 * q, 1), pltpu.roll(second, size - q, 1)]
    return jnp.concatenate(rows, axis=0)


def panel_steps(work, begin, end):
    def body(step, carry):
        panel_step(work, step)
        return carry

    lax.fori_loop(begin, end, body, 0)


def lower_of(work):
    shape = work.shape
    below = lax.broadcasted_iota(jnp.int32, shape, 1) <= lax.broadcasted_iota(jnp.int32, shape, 0)
    return jnp.where(below, work[...], 0.0)


def kernel(
    n, experts, entries, g_hbm, b_hbm, loads, flags, fresh, rot, pair, cross,
    g_ref, b_ref, bt, part, land, full, inner, rough, power, part2, land2,
    gram_a, gram_a_land, gram_b, gram_b_land, work, total, total_land,
    g_sem, b_sem,
    s_rs, r_rs, s_ag, r_ag, s_rs2, r_rs2, s_gr, r_gr, s_tot, r_tot,
):
    _, depth, block = g_ref.shape
    bits = n.bit_length() - 1
    expert_bits = experts.bit_length() - 1
    size = b_ref.shape[1]
    half = size // 2
    sub = half // 2
    me = lax.axis_index("row")
    my_expert = lax.axis_index("expert")
    orders = [tuple(range(bits)), tuple(reversed(range(bits)))]
    cuts = g_sem.shape[0] - n + 1

    def other(index, mask):
        at = index
        for bit in range(max(bits, expert_bits)):
            if mask >> bit & 1:
                at = at + (1 - 2 * (lax.rem(index // (1 << bit), 2))) * (1 << bit)
        return at

    def partner(bit):
        return {"row": other(me, 1 << bit), "expert": my_expert}

    def expert_partner(bit):
        return {"row": me, "expert": other(my_expert, 1 << bit)}

    place = my_expert // 2
    inside = jnp.logical_or(place == 1, place == 2)
    across = {"row": me, "expert": my_expert + jnp.where(place == 1, 2, -2)}
    if expert_bits == 3:
        rounds = [(SWAP, expert_partner(0)), (SWAP, expert_partner(1)), (ACROSS, across), (OUTWARD, expert_partner(1))]
    else:
        rounds = [(SWAP, expert_partner(b)) for b in range(expert_bits)]
    rounds = rounds + [(SWAP, partner(b)) for b in range(bits)]
    barrier = pltpu.get_barrier_semaphore()

    def greet(peer):
        pl.semaphore_signal(barrier, inc=1, device_id=peer, device_id_type=pl.DeviceIdType.MESH)

    greetings = 0
    for kind, peer in rounds:
        if kind == SWAP:
            greet(peer)
            greetings += 1
    if expert_bits == 3:
        pl.when(inside)(lambda: greet(across))
        greetings = greetings + inside.astype(jnp.int32)

    def load(index, cut=0):
        m = wanted[index]
        width = block if index else block // cuts
        columns = pl.ds(pl.multiple_of(other(me, m) * block + cut * width, width), width)
        sem = g_sem.at[cuts - 1 + index if index else cut]
        return pltpu.make_async_copy(g_hbm.at[:, columns], g_ref.at[m, :, pl.ds(cut * width, width)], sem)

    def load_basis(a):
        columns = pl.ds(a * half, half)
        return pltpu.make_async_copy(b_hbm.at[:, columns], b_ref.at[:, columns], b_sem.at[a])

    def copy(src, dst, send, recv, to):
        return pltpu.make_async_remote_copy(
            src_ref=src, dst_ref=dst, send_sem=send, recv_sem=recv,
            device_id=to, device_id_type=pl.DeviceIdType.MESH,
        )

    def settle(sent, sem):
        pltpu.make_async_copy(sent, sent, sem).wait()

    def strip(h):
        return pl.ds(h * sub, sub)

    schedule = []
    for phase in range(bits):
        lanes = []
        for h in range(2):
            order = orders[h]
            masks = [m for m in range(n) if first_bit(m, order) == phase]
            masks.sort(key=lambda m: first_bit(m & ~(1 << order[phase]), order))
            lanes.append([(h, phase, m, m & ~(1 << order[phase])) for m in masks])
        schedule.append([move for pair in zip(*lanes) for move in pair])
    slot = {}
    for phase_moves in schedule:
        for h, phase, m, there in phase_moves:
            slot[h, phase, there] = len(slot)

    def stage(h, m):
        return first_bit(m, orders[h]) % bits

    stages = [stage(h, there) for h, _, there in slot]

    class Halving:
        def __init__(self, a, parts, lands, sends, recvs, early):
            self.a, self.parts, self.lands, self.sends, self.recvs = a, parts, lands, sends, recvs
            self.early = early
            self.landed = set()

        def make(self, h, phase, m, there):
            at = slot[h, phase, there]
            count = cuts if self.early and (h, phase, m, there) in schedule[0][:2] else 1
            width = block // count
            return [
                copy(
                    self.parts.at[self.a, m, strip(h), pl.ds(cut * width, width)],
                    self.lands.at[self.a, at, :, pl.ds(cut * width, width)],
                    self.sends.at[self.a], self.recvs.at[self.a, stage(h, there)], partner(orders[h][phase]),
                )
                for cut in range(count)
            ]

        def absorb(self, h, phase, m):
            group = stage(h, m)
            if group not in self.landed:
                self.landed.add(group)
                settle(land.at[0, pl.ds(0, stages.count(group))], self.recvs.at[self.a, group])
            rows = slice(h * sub, (h + 1) * sub)
            self.parts[self.a, m, rows] = self.parts[self.a, m, rows] + self.lands[self.a, slot[h, phase, m]]

        def send(self, moves):
            for move in moves:
                for item in self.make(*move):
                    item.start()

        def forward(self):
            for phase in range(1, bits):
                for move in schedule[phase]:
                    for earlier in range(phase):
                        self.absorb(move[0], earlier, move[2])
                    self.send([move])

        def finish(self):
            for phase in range(bits):
                for h in range(2):
                    self.absorb(h, phase, 0)

        def drain(self):
            settle(self.parts.at[self.a, pl.ds(0, n - 1)], self.sends.at[self.a])

    first = [Halving(a, part, land, s_rs, r_rs, a == 0) for a in range(2)]
    second = [Halving(a, part2, land2, s_rs2, r_rs2, False) for a in range(2)]

    spread = []
    for h in range(2):
        held = [0]
        for bit in reversed(orders[h]):
            for m in list(held):
                spread.append((h, bit, m))
                held.append(m | 1 << bit)
    passed = {(h, m) for h, _, m in spread}
    groups = {}
    for h, bit, m in spread:
        there = m | 1 << bit
        level = bin(there).count("1")
        groups[h, there] = 2 * level - 2 + ((h, there) not in passed)
    names = sorted(set(groups.values()))
    groups = {key: names.index(value) for key, value in groups.items()}
    own = [item for pair in zip(*[[s for s in spread if s[0] == h and s[2] == 0] for h in range(2)]) for item in pair]
    relayed = sorted((s for s in spread if s[2]), key=lambda s: bin(s[2]).count("1"))

    def spread_copy(a, h, bit, m):
        src = part.at[a, 0, strip(h)] if m == 0 else full.at[a, m, strip(h)]
        return copy(src, full.at[a, m | 1 << bit, strip(h)], s_ag.at[a], r_ag.at[a, groups[h, m | 1 << bit]], partner(bit))

    arrived = set()

    def take(a, h, m):
        if m and (a, groups[h, m]) not in arrived:
            arrived.add((a, groups[h, m]))
            count = list(groups.values()).count(groups[h, m])
            settle(land.at[0, pl.ds(0, count)], r_ag.at[a, groups[h, m]])

    def relay(a):
        for h, bit, m in relayed:
            take(a, h, m)
            spread_copy(a, h, bit, m).start()

    tile = 256 if depth % 256 == 0 else 64
    masks = sorted(range(n), key=lambda v: bin(v).count("1"))

    largest = {}

    def add_power(a, m):
        for h in range(2):
            take(a, h, m)
        held = part[a, 0] if m == 0 else full[a, m]
        inner[a, m] = held.astype(BF16)
        peak = jnp.max(jnp.abs(held), axis=0, keepdims=True)
        largest[a] = peak if m == 0 else jnp.maximum(largest[a], peak)
        if m == masks[-1]:
            scale = scale_of(jnp.max(largest[a], axis=1, keepdims=True))
        for at in range(0, depth, tile):
            rows = slice(at, at + tile)
            term = dot_t(inner[a, m], g_ref[m, rows, :])
            if m:
                term = rough[a, :, rows] + term
            if m == masks[-1]:
                power[a * half : (a + 1) * half, rows] = (term * scale).astype(BF16)
            else:
                rough[a, :, rows] = term

    grams = [(gram_a, gram_a_land), (gram_b, gram_b_land)]

    def gram_copy(a, phase, h):
        held, landed = grams[a]
        extent = held.shape[1] // 2
        rows = pl.ds(h * extent, extent)
        return copy(
            held.at[phase, rows], landed.at[phase, rows],
            s_gr.at[a], r_gr.at[a, phase], partner(orders[h][phase]),
        )

    def gram_send(a, phase):
        for h in range(2):
            gram_copy(a, phase, h).start()

    def gram_add(a, phase):
        held, landed = grams[a]
        settle(landed.at[phase], r_gr.at[a, phase])
        held[phase + 1] = held[phase] + landed[phase]

    def total_copy(at):
        return copy(total.at[at], total_land.at[at], s_tot.at[0], r_tot.at[at], rounds[at][1])

    def total_start(at):
        if at == len(rounds):
            return
        if rounds[at][0] == SWAP:
            total_copy(at).start()
        else:
            pl.when(inside)(lambda: total_copy(at).start())

    def total_next(at):
        if at >= len(rounds):
            return
        kind = rounds[at][0]

        def add():
            total_copy(at).wait()
            total[at + 1] = total[at] + total_land[at]

        def give():
            total_copy(at).wait_send()
            total[at + 1] = total[at]

        def accept():
            total_copy(at).wait_recv()
            total[at + 1] = total_land[at]

        if kind == SWAP:
            add()
        elif kind == ACROSS:
            pl.when(inside)(add)
        else:
            pl.when(inside)(give)
            pl.when(jnp.logical_not(inside))(accept)
        total_start(at + 1)

    wanted = [move[2] for move in schedule[0]] + list(range(n))
    wanted = sorted(range(n), key=wanted.index)
    load_basis(0).start()
    for cut in range(cuts):
        load(0, cut).start()
    span = 128 if depth % 128 == 0 else depth

    def turn_basis(a):
        for at in range(0, depth, span):
            bt[a * half : (a + 1) * half, at : at + span] = b_ref[at : at + span, a * half : (a + 1) * half].T

    load_basis(0).wait()
    for index in range(1, n):
        load(index).start()
    load_basis(1).start()
    turn_basis(0)

    def inner_part(a, m):
        part[a, m] = dot(bt[a * half : (a + 1) * half, :], g_ref[m])

    opening = schedule[0][:2]
    rest = schedule[0][2:]
    for cut in range(cuts):
        load(0, cut).wait()
        columns = slice(cut * (block // cuts), (cut + 1) * (block // cuts))
        part[0, wanted[0], :, columns] = dot(bt[:half, :], g_ref[wanted[0], :, columns])
        if cut == 0:
            pl.semaphore_wait(barrier, greetings)
        for move in opening:
            first[0].make(*move)[cut].start()
    for index in range(1, n):
        load(index).wait()
        m = wanted[index]
        if m == wanted[-1]:
            load_basis(1).wait()
            turn_basis(1)
            inner_part(1, wanted[0])
            first[1].send(opening)
        inner_part(0, m)
        first[0].send([move for move in rest if move[2] == m])
    for m in wanted[1:]:
        inner_part(1, m)
    live = loads[0] >= 1
    refresh = jnp.logical_and(live, flags[0] == 1)
    first[0].forward()
    first[1].send(rest)

    def squares_of(step, sums):
        rows = pl.ds(pl.multiple_of(step * 16, 16), 16)
        for m in range(n):
            piece = g_ref[m, rows, :].astype(F32)
            sums = sums + piece * piece
        return sums

    sums = lax.fori_loop(0, depth // 16, squares_of, jnp.zeros((16, block), F32))
    total_sq = jnp.where(live, jnp.sum(sums), 0.0)
    count = jnp.where(jnp.logical_and(live, me == 0), 1.0, 0.0)
    lane = lax.broadcasted_iota(jnp.int32, (1, 128), 1)
    total[0] = jnp.where(lane == 0, total_sq, jnp.where(lane == 1, count, 0.0))
    total_start(0)
    first[1].forward()
    total_next(0)
    first[0].finish()
    for item in own:
        spread_copy(0, *item).start()
    add_power(0, 0)
    total_next(1)
    first[1].finish()
    for item in own[:2]:
        spread_copy(1, *item).start()
    total_next(2)
    add_power(1, 0)
    relay(0)
    for item in own[2:]:
        spread_copy(1, *item).start()
    relay(1)
    total_next(3)
    for m in masks[1:]:
        add_power(0, m)
    gram_a[0] = pack(dot_t(power[0:half, :], power[0:half, :]))
    gram_send(0, 0)

    def cross_part(a):
        for m in wanted:
            part2[a, m] = dot(power[a * half : (a + 1) * half, :], g_ref[m])

    cross_part(0)
    second[0].send(opening)
    for m in masks[1:-1]:
        add_power(1, m)
    for phase in range(bits - 1):
        gram_add(0, phase)
        gram_send(0, phase + 1)
    add_power(1, masks[-1])
    total_next(4)
    gram_b[0, :half] = dot_t(power[:half, :], power[half:size, :])
    gram_b_square = dot_t(power[half:size, :], power[half:size, :])
    gram_b[0, half:] = pack(gram_b_square)
    gram_send(1, 0)
    second[0].send(rest)
    cross_part(1)
    gram_add(0, bits - 1)
    panels = half // PANEL
    work[...] = unpack(gram_a[bits])
    panel_steps(work, 0, panels // 4)
    for phase in range(bits - 1):
        gram_add(1, phase)
        gram_send(1, phase + 1)
    second[1].send(opening)
    second[0].forward()
    second[1].send(rest)
    panel_steps(work, panels // 4, panels)

    def write_fresh(a, pieces):
        for at in range(0, depth, tile):
            rows = slice(at, at + tile)
            columns = slice(a * half, (a + 1) * half)
            left = power[0 : (a + 1) * half, rows].T
            value = dot(left, pieces[2]) + dot(left, pieces[1]) + dot(left, pieces[0])
            kept = jnp.where(live, b_ref[rows, columns].astype(F32), 0.0)
            fresh[rows, columns] = jnp.where(refresh, value, kept)

    inverse_a = lower_of(work)
    write_fresh(0, pieces_of(inverse_a.T, 3))
    gram_add(1, bits - 1)
    upper = dot(inverse_a, gram_b[bits, :half], HIGHEST)
    work[...] = unpack(gram_b[bits, half:]) - dot(upper.T, upper, HIGHEST)
    panel_steps(work, 0, panels * 5 // 8)
    second[1].forward()
    panel_steps(work, panels * 5 // 8, panels)
    second[0].finish()
    turned_a = dot(inverse_a, part2[0, 0], HIGHEST)
    inverse_b = lower_of(work)
    mixed = -dot(inverse_b, dot(upper.T, inverse_a, HIGHEST), HIGHEST)
    write_fresh(1, pieces_of(jnp.concatenate([mixed, inverse_b], axis=1).T, 3))
    for at in range(5, len(rounds)):
        total_next(at)
    final = total[len(rounds)]
    norm = lax.rsqrt(final[0:1, 0:1] / (final[0:1, 1:2] * entries) + 1e-6)

    def write_rot(a, turned):
        rot[a * half : (a + 1) * half, :] = jnp.where(refresh, turned, jnp.where(live, part[a, 0], 0.0)) * norm

    write_rot(0, turned_a)
    write_rot(1, dot(mixed, part2[0, 0], HIGHEST))
    pair[...] = jnp.concatenate(pieces_of(jnp.where(refresh, inverse_b * norm, 0.0), 2), axis=1)
    second[1].finish()
    cross[...] = jnp.where(refresh, part2[1, 0], 0.0)
    for a in range(2):
        first[a].drain()
        second[a].drain()
        settle(full.at[a, pl.ds(0, n - 1)], s_ag.at[a])
        settle(grams[a][0].at[pl.ds(0, bits)], s_gr.at[a])


def write_out(fresh, rot, pair, cross, fresh_hbm, rot_hbm, last, fresh_sem, rot_sem):
    extent = fresh.shape[0] // PARTS
    half = cross.shape[0]
    copies = [pltpu.make_async_copy(rot.at[pl.ds(0, half)], rot_hbm.at[0, pl.ds(0, half)], rot_sem.at[0])]
    for at in range(PARTS):
        rows = pl.ds(at * extent, extent)
        copies.append(pltpu.make_async_copy(fresh.at[rows], fresh_hbm.at[0, rows], fresh_sem.at[at]))
    for item in copies:
        item.start()
    top, low = pieces_of(cross[...], 2)
    turned = dot(pair[...], jnp.concatenate([low, low], axis=0)) + dot(pair[...], jnp.concatenate([top, top], axis=0))
    last[...] = rot[half:, :] + turned
    copies.append(pltpu.make_async_copy(last, rot_hbm.at[0, pl.ds(half, half)], rot_sem.at[1]))
    copies[-1].start()
    for item in copies:
        item.wait()


def on_device(n, experts, grads, basis, loads, flags):
    _, depth, wide = grads.shape
    size = basis.shape[2]
    half = size // 2
    block = wide // n
    bits = n.bit_length() - 1
    rounds = bits + experts.bit_length() - 1 + (experts == 8)
    moves = 2 * (n - 1)
    packed = half * 5 // 8
    cuts = 2 if block % 256 == 0 else 1
    anywhere = pl.BlockSpec(memory_space=pl.ANY)
    vmem = pl.BlockSpec(memory_space=pltpu.VMEM)
    chunk = (half // 2, block)
    dma = pltpu.SemaphoreType.DMA
    results = pl.pallas_call(
        functools.partial(kernel, n, experts, float(depth * n * wide)),
        out_shape=(
            pltpu.VMEM((depth, size), F32), pltpu.VMEM((size, block), F32),
            pltpu.VMEM((half, size), BF16), pltpu.VMEM((half, block), F32),
        ),
        in_specs=[pl.BlockSpec(memory_space=pltpu.HBM)] * 2 + [pl.BlockSpec(memory_space=pltpu.SMEM)] * 2,
        out_specs=(vmem, vmem, vmem, vmem),
        scratch_shapes=[
            pltpu.VMEM((n, depth, block), BF16),
            pltpu.VMEM((depth, size), BF16),
            pltpu.VMEM((size, depth), BF16),
            pltpu.VMEM((2, n, half, block), F32),
            pltpu.VMEM((2, moves, *chunk), F32),
            pltpu.VMEM((2, n, half, block), F32),
            pltpu.VMEM((2, n, half, block), BF16),
            pltpu.VMEM((2, half, depth), F32),
            pltpu.VMEM((size, depth), BF16),
            pltpu.VMEM((2, n, half, block), F32),
            pltpu.VMEM((2, moves, *chunk), F32),
            pltpu.VMEM((bits + 1, packed, half), F32),
            pltpu.VMEM((bits, packed, half), F32),
            pltpu.VMEM((bits + 1, half + packed, half), F32),
            pltpu.VMEM((bits, half + packed, half), F32),
            pltpu.VMEM((half, half), F32),
            pltpu.VMEM((rounds + 1, 1, 128), F32),
            pltpu.VMEM((rounds, 1, 128), F32),
            dma((n - 1 + cuts,)), dma((2,)),
            dma((2,)), dma((2, bits)), dma((2,)), dma((2, 2 * bits - 1)), dma((2,)), dma((2, bits)),
            dma((2,)), dma((2, bits)), dma((1,)), dma((rounds,)),
        ],
        compiler_params=pltpu.CompilerParams(
            collective_id=0, has_side_effects=True, vmem_limit_bytes=32 * 1024 * 1024
        ),
    )(*[pltpu.with_memory_space_constraint(x, pltpu.HBM) for x in (grads[0], basis[0])], loads, flags)
    return pl.pallas_call(
        write_out,
        out_shape=(
            jax.ShapeDtypeStruct((1, depth, size), F32),
            jax.ShapeDtypeStruct((1, size, block), F32),
        ),
        in_specs=[vmem] * 4,
        out_specs=(anywhere, anywhere),
        scratch_shapes=[pltpu.VMEM((half, block), F32), dma((PARTS,)), dma((2,))],
        compiler_params=pltpu.CompilerParams(vmem_limit_bytes=16 * 1024 * 1024),
    )(*results)


def solution(mesh):
    placed = (P("expert", "row", None), P("expert", "row", None), P("expert"), P("expert"))
    return jax.shard_map(
        functools.partial(on_device, mesh.shape["row"], mesh.shape["expert"]),
        mesh=mesh,
        in_specs=placed,
        out_specs=(P("expert", "row", None), P("expert", None, "row")),
        check_vma=False,
    )
```
